32 devices in a mesh: dp: 2 (over core), seq: 8 (over z, x), mp: 2 (over y).
Axes of the slice: x: 2, y: 2, z: 4, core: 2. Of those that a mesh axis runs over, the one named last changes fastest.
Arguments:
- queries: bfloat16 [4, 1024, 4096], P('dp', 'seq', 'mp'), may hold values from -6 to 6
- vision: bfloat16 [4, 640, 4096], P('dp', 'seq'), may hold values from -6 to 6
- key_weight: bfloat16 [4096, 1024], P(None, 'mp'), may hold values from -0.09375 to 0.09375
- value_weight: bfloat16 [4096, 1024], P(None, 'mp'), may hold values from -0.09375 to 0.09375
- query_gain: float32 [128], replicated, may hold values from 0.6 to 6
- key_gain: float32 [128], replicated, may hold values from 0.6 to 6
- out_grad: bfloat16 [4, 1024, 4096], P('dp', 'seq', 'mp'), may hold values from -6 to 6
- tile_count: int32 [4], P('dp'), may hold values from 1 to 4, as said below
Outputs:
- query_grad: bfloat16 [4, 1024, 4096], P('dp', 'seq', 'mp')
- vision_grad: bfloat16 [4, 640, 4096], P('dp', 'seq', 'mp')
- key_weight_grad: float32 [4096, 1024], P(None, 'mp')
- value_weight_grad: float32 [4096, 1024], P(None, 'mp')
The draws below stay inside these ranges and needn't reach their ends.
Inputs may be any that keep to these rules, and one draw needn't show every extreme that they name: The live vision tokens of sample s are its first tile_count[s] * 160; some sample has 4 tiles and some other sample has 1.
All inputs are finite; a program needn't handle non-finite values.
Results may differ from the reference program's by a relative error of at most 0.03.
The reference program's roundings to bfloat16 on the way (of `keys`, `values`, `normed`, `probs_b`, `attn`, `dscores`, `key_grad` and `value_grad`) count: a program that leaves them out, or rounds other values in their place, can miss the bound.
Values may be sent and summed in bfloat16 or wider, within the bound.
No kernel may reach another device: no remote copies, remote signals or barrier semaphores. Data moves between devices by JAX's collectives and lax.ppermute only.
A program may use at most 128 MiB of HBM per device.

```python
import jax
import jax.numpy as jnp
from jax import lax

D = 4096
HEADS = 32
KV_HEADS = 8
HEAD_DIM = 128
MAX_TILES = 4
SAMPLES = 4
TXT = 1024
VIS = 640
TILE_TOK = 160


def vision_field(key):
    drawn = jax.random.normal(jax.random.fold_in(key, 7001), (SAMPLES, VIS, D), jnp.float32)
    return jnp.clip(drawn, -6.0, 6.0)


def key_matrix(key):
    drawn = jax.random.normal(jax.random.fold_in(key, 7002), (D, KV_HEADS * HEAD_DIM), jnp.float32)
    return jnp.clip(drawn, -6.0, 6.0) * D ** (-0.5)


def draw_vision(key, part):
    return vision_field(key).astype(jnp.bfloat16)


def draw_key_weight(key, part):
    return key_matrix(key).astype(jnp.bfloat16)


def draw_queries(key, part):
    drawn = jax.random.normal(jax.random.fold_in(key, 7003), (SAMPLES, TXT, HEADS * HEAD_DIM), jnp.float32)
    drawn = jnp.clip(drawn, -6.0, 6.0)
    return drawn.astype(jnp.bfloat16)


def draw_query_gain(key, part):
    inner = jax.random.fold_in(key, 7005)
    return jax.random.uniform(inner, (HEAD_DIM,), jnp.float32, 0.6, 1.4)


def draw_key_gain(key, part):
    inner = jax.random.fold_in(key, 7006)
    return jax.random.uniform(inner, (HEAD_DIM,), jnp.float32, 0.6, 1.4)


def draw_tile_count(key, part):
    counts = jax.random.randint(jax.random.fold_in(key, 7101), (SAMPLES,), 1, MAX_TILES + 1, dtype=jnp.int32)
    full_at = jax.random.randint(jax.random.fold_in(key, 7102), (), 0, SAMPLES, dtype=jnp.int32)
    step_to = jax.random.randint(jax.random.fold_in(key, 7103), (), 1, SAMPLES, dtype=jnp.int32)
    single_at = (full_at + step_to) % SAMPLES
    counts = counts.at[full_at].set(MAX_TILES)
    counts = counts.at[single_at].set(1)
    return counts.astype(jnp.int32)


def steps_of(stream_key, extent, pieces, smallest, top_value):
    def one(dim, shards_of):
        heights = jax.random.uniform(jax.random.fold_in(jax.random.fold_in(stream_key, 6), dim), (shards_of,), jnp.float32, smallest / len(pieces), top_value / len(pieces))
        return jnp.repeat(jnp.exp(heights), extent[dim] // shards_of).reshape((-1,) + (1,) * (len(extent) - dim - 1))

    level = one(*pieces[0])
    for cut in pieces[1:]:
        level = level * one(*cut)
    return level


def noise(own_key, dims, scale, bound, split=(), kind=jnp.bfloat16):
    values = jax.random.normal(own_key, dims, jnp.float32) * scale
    if len(split) > 0:
        values = steps_of(own_key, dims, split, -0.22, 0.18) * values
    return jnp.clip(values, min=-bound, max=bound).astype(kind)


def setup_inputs(seed: int = 0) -> dict:
    key_of = jax.random.split(jax.random.key(seed), 9)
    queries = draw_queries(jax.random.fold_in(key_of[8], 71), 0)
    vision = draw_vision(jax.random.fold_in(key_of[8], 71), 0)
    key_weight = draw_key_weight(jax.random.fold_in(key_of[8], 71), 0)
    value_weight = noise(key_of[3], (D, KV_HEADS * HEAD_DIM), D ** -0.5, 0.09375, ((1, 2),))
    query_gain = draw_query_gain(jax.random.fold_in(key_of[8], 71), 0)
    key_gain = draw_key_gain(jax.random.fold_in(key_of[8], 71), 0)
    out_grad = noise(key_of[6], (SAMPLES, TXT, HEADS * HEAD_DIM), 1.0, 6.0, ((0, 2), (1, 8), (2, 2)))
    tile_count = draw_tile_count(jax.random.fold_in(key_of[8], 71), 0)
    return {"queries": queries, "vision": vision, "key_weight": key_weight, "value_weight": value_weight, "query_gain": query_gain, "key_gain": key_gain, "out_grad": out_grad, "tile_count": tile_count}


EPS = 1e-05
NEG = -1e+30

def norm_apply(raw, gain):
    inverse = lax.rsqrt(lax.optimization_barrier(jnp.mean(raw * raw, axis=-1, keepdims=True)) + EPS)
    return (raw * inverse * gain, inverse)

def norm_back(raw, inverse, gain, upstream):
    weighted = upstream * gain
    return inverse * weighted - raw * inverse * inverse * inverse * lax.optimization_barrier(jnp.mean(weighted * raw, axis=-1, keepdims=True))

def sample_grads(queries_one, vision_one, out_one, tiles_one, key_weight, value_weight, query_gain, key_gain):
    group_size = HEADS // KV_HEADS
    score_scale = HEAD_DIM ** (-0.5)
    key_cols = key_weight.reshape(D, KV_HEADS, HEAD_DIM).transpose(1, 0, 2)
    value_cols = value_weight.reshape(D, KV_HEADS, HEAD_DIM).transpose(1, 0, 2)
    query_heads = queries_one.reshape(TXT, KV_HEADS, group_size, HEAD_DIM).transpose(1, 0, 2, 3)
    out_heads = out_one.reshape(TXT, KV_HEADS, group_size, HEAD_DIM).transpose(1, 0, 2, 3)
    live_keys = jnp.arange(VIS, dtype=jnp.int32) < tiles_one * TILE_TOK

    def one_group(vision_total, inputs):
        key_col, value_col, query_group, out_group = inputs
        key_raw = jnp.dot(vision_one, key_col, preferred_element_type=jnp.float32)
        key_normed, key_inverse = norm_apply(key_raw, key_gain)
        keys = key_normed.astype(jnp.bfloat16)
        values = jnp.dot(vision_one, value_col, preferred_element_type=jnp.float32).astype(jnp.bfloat16)
        query_raw = query_group.astype(jnp.float32)
        query_normed, query_inverse = norm_apply(query_raw, query_gain)
        normed = query_normed.astype(jnp.bfloat16)
        normed_wide = normed.astype(jnp.float32)
        keys_wide = keys.astype(jnp.float32)
        values_wide = values.astype(jnp.float32)
        out_wide = out_group.astype(jnp.float32)
        scores = jnp.einsum('tgd,jd->gtj', normed_wide, keys_wide) * score_scale
        scores = jnp.where(live_keys[None, None, :], scores, NEG)
        row_top = lax.optimization_barrier(jnp.max(scores, axis=-1, keepdims=True))
        expo = jnp.exp(scores - row_top)
        probs = expo / lax.optimization_barrier(jnp.sum(expo, axis=-1, keepdims=True))
        probs_b = probs.astype(jnp.bfloat16)
        probs_wide = probs_b.astype(jnp.float32)
        attn = jnp.einsum('gtj,jd->tgd', probs_wide, values_wide).astype(jnp.bfloat16)
        delta = lax.optimization_barrier(jnp.sum(out_wide * attn.astype(jnp.float32), axis=-1))
        dprobs = jnp.einsum('tgd,jd->gtj', out_wide, values_wide)
        dscores = (probs * (dprobs - delta.T[:, :, None])).astype(jnp.bfloat16)
        dscores_wide = dscores.astype(jnp.float32)
        dnormed = jnp.einsum('gtj,jd->tgd', dscores_wide, keys_wide) * score_scale
        dkeys = jnp.einsum('gtj,tgd->jd', dscores_wide, normed_wide) * score_scale
        dvalues = jnp.einsum('gtj,tgd->jd', probs_wide, out_wide)
        query_part = norm_back(query_raw, query_inverse, query_gain, dnormed).astype(jnp.bfloat16)
        key_grad = norm_back(key_raw, key_inverse, key_gain, dkeys).astype(jnp.bfloat16)
        value_grad = dvalues.astype(jnp.bfloat16)
        key_weight_part = jnp.dot(vision_one.T, key_grad, preferred_element_type=jnp.float32)
        value_weight_part = jnp.dot(vision_one.T, value_grad, preferred_element_type=jnp.float32)
        vision_term = jnp.dot(key_grad, key_col.T, preferred_element_type=jnp.float32)
        vision_term = vision_term + jnp.dot(value_grad, value_col.T, preferred_element_type=jnp.float32)
        return (vision_total + vision_term, (query_part, key_weight_part, value_weight_part))
    start_total = jnp.zeros((VIS, D), jnp.float32)
    vision_total, stacked = lax.scan(one_group, start_total, (key_cols, value_cols, query_heads, out_heads))
    query_parts, key_parts, value_parts = stacked
    query_grad = query_parts.transpose(1, 0, 2, 3).reshape(TXT, HEADS * HEAD_DIM)
    key_weight_part = key_parts.transpose(1, 0, 2).reshape(D, KV_HEADS * HEAD_DIM)
    value_weight_part = value_parts.transpose(1, 0, 2).reshape(D, KV_HEADS * HEAD_DIM)
    return (query_grad, vision_total.astype(jnp.bfloat16), key_weight_part, value_weight_part)

def reference(queries, vision, key_weight, value_weight, query_gain, key_gain, out_grad, tile_count):
    query_list = []
    vision_list = []
    key_weight_grad = jnp.zeros((D, KV_HEADS * HEAD_DIM), jnp.float32)
    value_weight_grad = jnp.zeros((D, KV_HEADS * HEAD_DIM), jnp.float32)
    for sample_at in range(SAMPLES):
        query_part, vision_part, key_part, value_part = sample_grads(queries[sample_at], vision[sample_at], out_grad[sample_at], tile_count[sample_at], key_weight, value_weight, query_gain, key_gain)
        query_list.append(query_part)
        vision_list.append(vision_part)
        key_weight_grad = key_weight_grad + key_part
        value_weight_grad = value_weight_grad + value_part
    return (jnp.stack(query_list), jnp.stack(vision_list), key_weight_grad, value_weight_grad)
```

```python
import functools
import math

import jax
import jax.numpy as jnp
from jax import lax
from jax.experimental import pallas as pl
from jax.experimental.pallas import tpu as pltpu
from jax.sharding import PartitionSpec as P

MAX_TILES = 4
EPS = 1e-05
NEG = -1e30
F32 = jnp.float32
BF16 = jnp.bfloat16


def attention_kernel(blocks, parts, group, head_dim, scalars, gain_ref, *refs):
    q_refs, refs = refs[:parts], refs[parts:]
    g_refs, refs = refs[:parts], refs[parts:]
    kv_refs, refs = refs[:blocks], refs[blocks:]
    dq_refs, refs = refs[:parts], refs[parts:]
    dkv_refs, refs = refs[:blocks], refs[blocks:]
    keys, values, dkeys, dvalues = refs
    rows = kv_refs[0].shape[0]
    total = rows * blocks
    scale = head_dim ** (-0.5)
    column = lax.broadcasted_iota(jnp.int32, (1, total), 1)
    live = column < 0
    for k in range(blocks):
        keys[k * rows : (k + 1) * rows, :] = kv_refs[k][:, :head_dim]
        values[k * rows : (k + 1) * rows, :] = kv_refs[k][:, head_dim:]
        start = k * rows
        live = live | ((column >= start) & (column < start + scalars[1 + k]))
    bias = jnp.where(live, 0.0, NEG)
    gain = gain_ref[...]
    keys_all = keys[...]
    values_all = values[...]
    for h in range(group):
        cols = slice(h * head_dim, (h + 1) * head_dim)
        raw_b = jnp.concatenate([ref[..., cols].reshape(-1, head_dim) for ref in q_refs], axis=0)
        out_b = jnp.concatenate([ref[..., cols].reshape(-1, head_dim) for ref in g_refs], axis=0)
        raw = raw_b.astype(F32)
        inverse = lax.rsqrt(jnp.mean(raw * raw, axis=-1, keepdims=True) + EPS)
        unit = raw * inverse
        normed = (unit * gain).astype(BF16)
        scores = lax.dot_general(normed, keys_all, (((1,), (1,)), ((), ())), preferred_element_type=F32)
        scores = scores * (scale * math.log2(math.e)) + bias
        expo = jnp.exp2(scores - jnp.max(scores, axis=-1, keepdims=True))
        probs = expo * (1.0 / jnp.sum(expo, axis=-1, keepdims=True))
        probs_b = probs.astype(BF16)
        attn = jnp.dot(probs_b, values_all, preferred_element_type=F32).astype(BF16)
        delta = jnp.sum(out_b.astype(F32) * attn.astype(F32), axis=-1, keepdims=True)
        dprobs = lax.dot_general(out_b, values_all, (((1,), (1,)), ((), ())), preferred_element_type=F32)
        dscores = (probs * (dprobs - delta)).astype(BF16)
        dnormed = jnp.dot(dscores, keys_all, preferred_element_type=F32) * scale
        weighted = dnormed * gain
        grad = inverse * (weighted - unit * jnp.mean(weighted * unit, axis=-1, keepdims=True))
        grad = grad.astype(BF16)
        part_rows = grad.shape[0] // parts
        for p in range(parts):
            dq_refs[p][:, cols] = grad[p * part_rows : (p + 1) * part_rows]
        over_rows = (((0,), (0,)), ((), ()))
        dk = lax.dot_general(dscores, normed, over_rows, preferred_element_type=F32)
        dv = lax.dot_general(probs_b, out_b, over_rows, preferred_element_type=F32)
        if h == 0:
            dkeys[...] = dk
            dvalues[...] = dv
        else:
            dkeys[...] += dk
            dvalues[...] += dv
    for k in range(blocks):
        span = slice(k * rows, (k + 1) * rows)
        dkv_refs[k][:, :head_dim] = (dkeys[span, :] * scale).astype(BF16)
        dkv_refs[k][:, head_dim:] = dvalues[span, :].astype(BF16)


def attention(scalars, gain, queries, other_queries, out_grad, other_grads, kv_blocks, head_dim):
    blocks = len(kv_blocks)
    parts = 1 + len(other_queries)
    text_rows, width = queries.shape[1:]
    rows, kv_width = kv_blocks[0].shape
    kv_here = kv_width // (2 * head_dim)
    group = width // head_dim // kv_here
    group_width = group * head_dim
    total = rows * blocks
    own = pl.BlockSpec((1, text_rows, group_width), lambda g, s: (s[0], 0, g))
    other = pl.BlockSpec((text_rows, group_width), lambda g, s: (0, g))
    kv = pl.BlockSpec((rows, 2 * head_dim), lambda g, s: (0, g))
    gain_spec = pl.BlockSpec((1, head_dim), lambda g, s: (0, 0))
    work = text_rows * parts * group * kv_here * total
    results = pl.pallas_call(
        functools.partial(attention_kernel, blocks, parts, group, head_dim),
        grid_spec=pltpu.PrefetchScalarGridSpec(
            num_scalar_prefetch=1,
            grid=(kv_here,),
            in_specs=[gain_spec] + ([own] + [other] * (parts - 1)) * 2 + [kv] * blocks,
            out_specs=[other] * parts + [kv] * blocks,
            scratch_shapes=[pltpu.VMEM((total, head_dim), BF16)] * 2
            + [pltpu.VMEM((total, head_dim), F32)] * 2,
        ),
        out_shape=[jax.ShapeDtypeStruct((text_rows, width), BF16)] * parts
        + [jax.ShapeDtypeStruct((rows, kv_width), BF16)] * blocks,
        cost_estimate=pl.CostEstimate(
            flops=12 * work * head_dim, bytes_accessed=6 * text_rows * parts * width, transcendentals=work
        ),
        name="attention",
    )(scalars, gain.reshape(1, head_dim), queries, *other_queries, out_grad, *other_grads, *kv_blocks)
    return results[:parts], results[parts:]


def scatter_kernel(pieces, starts, *refs):
    piece_refs, refs = refs[:pieces], refs[pieces:]
    key_out, value_out = refs[2], refs[3]
    wide, sem = refs[4], refs[5]
    half = key_out.shape[1]
    copies = []
    at = 0
    for p in range(pieces):
        rows = piece_refs[p].shape[0]
        for q, out in enumerate((key_out, value_out)):
            wide[q, at : at + rows, :] = piece_refs[p][:, q * half : (q + 1) * half].astype(F32)
            start = pl.multiple_of(starts[p], 8)
            copy = pltpu.make_async_copy(
                wide.at[q, pl.ds(at, rows), :], out.at[pl.ds(start, rows), :], sem.at[p, q]
            )
            copy.start()
            copies.append(copy)
        at += rows
    for copy in copies:
        copy.wait()


def scatter_rows(outs, pieces, starts):
    count = len(pieces)
    rows = sum(p.shape[0] for p in pieces)
    width = pieces[0].shape[1] // 2
    return pl.pallas_call(
        functools.partial(scatter_kernel, count),
        grid_spec=pltpu.PrefetchScalarGridSpec(
            num_scalar_prefetch=1,
            grid=(1,),
            in_specs=[pl.BlockSpec(p.shape, lambda i, s: (0, 0)) for p in pieces]
            + [pl.BlockSpec(memory_space=pl.ANY)] * 2,
            out_specs=[pl.BlockSpec(memory_space=pl.ANY)] * 2,
            scratch_shapes=[pltpu.VMEM((2, rows, width), F32), pltpu.SemaphoreType.DMA((count, 2))],
        ),
        out_shape=[jax.ShapeDtypeStruct(o.shape, F32) for o in outs],
        input_output_aliases={1 + count: 0, 2 + count: 1},
        cost_estimate=pl.CostEstimate(flops=rows * width * 2000, bytes_accessed=rows * width * 12, transcendentals=0),
        name="scatter_rows",
    )(jnp.stack(starts).astype(jnp.int32), *pieces, *outs)


def blank_kernel(*refs):
    pass


def blank(shape):
    return pl.pallas_call(
        blank_kernel,
        out_specs=[pl.BlockSpec(memory_space=pl.ANY)] * 2,
        out_shape=[jax.ShapeDtypeStruct(shape, F32)] * 2,
        name="blank",
    )()


def norm_apply(raw, gain):
    inverse = lax.rsqrt(jnp.mean(raw * raw, axis=-1, keepdims=True) + EPS)
    return (raw * inverse * gain, inverse)


def norm_back(raw, inverse, gain, upstream):
    weighted = upstream * gain
    return inverse * weighted - raw * inverse * inverse * inverse * jnp.mean(
        weighted * raw, axis=-1, keepdims=True
    )


def local(sizes, queries, vision, key_weight, value_weight, query_gain, key_gain, out_grad, tile_count):
    n, dps, mps = sizes["seq"], sizes["dp"], sizes["mp"]
    head_dim = query_gain.shape[0]
    samples, rows, model = vision.shape
    width = key_weight.shape[1]
    kv_here = width // head_dim
    me, mine, mp = lax.axis_index("seq"), lax.axis_index("dp"), lax.axis_index("mp")
    x = me % samples
    pair = me // samples * samples
    order = [i for i in range(0, n, 2)] + [i for i in range(n - 1, 0, -2)]
    place = [order.index(i) for i in range(n)]
    at = jnp.array(place, jnp.int32)[me]

    def shift(value, k):
        return lax.ppermute(value, "seq", [(i, (i + k) % n) for i in range(n)])

    def ring(value, k):
        return lax.ppermute(value, "seq", [(order[i], order[(i + k) % n]) for i in range(n)])

    def within(value, k):
        perm = [(i, i // samples * samples + (i % samples + k) % samples) for i in range(n)]
        return lax.ppermute(value, "seq", perm)

    def relative(value):
        return [lax.dynamic_index_in_dim(value, (x + r) % samples, 0, False) for r in range(samples)]

    flat_vision = vision.reshape(samples * rows, model)
    key_raw = jnp.dot(flat_vision, key_weight, preferred_element_type=F32)
    key_raw = key_raw.reshape(samples, rows, kv_here, head_dim)
    key_normed, key_inverse = norm_apply(key_raw, key_gain)
    own_values = jnp.dot(flat_vision, value_weight, preferred_element_type=F32)
    own_values = own_values.astype(BF16).reshape(samples, rows, kv_here, head_dim)
    own_kv = jnp.stack([key_normed.astype(BF16), own_values], axis=3)
    own_kv = own_kv.reshape(samples, rows, 2 * width)
    kv_rel = relative(own_kv)
    kv_blocks = [kv_rel[0]] + [shift(kv_rel[k % samples], k) for k in range(1, n)]
    other_queries = [within(lax.dynamic_index_in_dim(queries, (x + r) % samples, 0, False), r) for r in range(1, samples)]
    other_grads = [within(lax.dynamic_index_in_dim(out_grad, (x + r) % samples, 0, False), r) for r in range(1, samples)]
    tile_rows = n * rows // MAX_TILES
    live_end = tile_count[x] * tile_rows
    source = (me - jnp.arange(n, dtype=jnp.int32)) % n
    live = jnp.clip(live_end - source * rows, 0, rows)
    scalars = jnp.concatenate([x[None], live]).astype(jnp.int32)
    dq, dkv = attention(scalars, query_gain, queries, other_queries, out_grad, other_grads, kv_blocks, head_dim)

    share = model // n
    vision_blocks = []
    for k in range(n):
        cut = lax.dynamic_slice_in_dim(flat_vision, (at + k) % n * share, share, axis=1)
        vision_blocks.append(cut if k == 0 else ring(cut, k))

    arrived = [dkv[0]] + [shift(dkv[k], -k) for k in range(1, n)]
    sums = []
    for r in range(samples):
        total = arrived[r].astype(F32)
        for k in range(r + samples, n, samples):
            total = total + arrived[k].astype(F32)
        sums.append(total)
    sums = jnp.stack([lax.select_n((s - x) % samples, *sums) for s in range(samples)])
    sums = sums.reshape(samples, rows, kv_here, 2, head_dim)
    key_grad = norm_back(key_raw, key_inverse, key_gain, sums[:, :, :, 0]).astype(BF16)
    value_grad = sums[:, :, :, 1].astype(BF16)
    key_grad = key_grad.reshape(samples * rows, width)
    value_grad = value_grad.reshape(samples * rows, width)
    own_grads = jnp.concatenate([key_grad, value_grad], axis=1)

    def ring_gather(value):
        half = value.shape[0] // 2
        got = [value] + [None] * (n - 1)
        up = down = value
        for k in range(1, n // 2):
            up, down = ring(up, 1), ring(down, -1)
            got[k], got[n - k] = up, down
        got[n // 2] = (ring(up[:half], 1), ring(down[half:], -1))
        return got

    grad_blocks = ring_gather(own_grads)
    grad_blocks[n // 2] = jnp.concatenate(grad_blocks[n // 2], axis=0)
    part = lax.dot_general(
        jnp.concatenate(vision_blocks, axis=0),
        jnp.concatenate(grad_blocks, axis=0),
        (((0,), (0,)), ((), ())),
        preferred_element_type=F32,
    )
    piece = share // dps
    shard = lax.dynamic_slice_in_dim(part, mine * piece, piece, axis=0)
    for k in range(1, dps):
        sent = lax.dynamic_slice_in_dim(part, (mine + k) % dps * piece, piece, axis=0)
        got = lax.ppermute(sent.astype(BF16), "dp", [(i, (i + k) % dps) for i in range(dps)])
        shard = shard + got.astype(F32)
    shard = shard.astype(BF16)

    def both(values, starts):
        pieces, where = list(values), [s + mine * piece for s in starts]
        for k in range(1, dps):
            perm = [(i, (i + k) % dps) for i in range(dps)]
            pieces += [lax.ppermute(v, "dp", perm) for v in values]
            where += [s + (mine - k) % dps * piece for s in starts]
        return pieces, where

    outs = blank((model, width))
    outs = scatter_rows(outs, *both([shard], [at * share]))
    shards = ring_gather(shard)
    for k in range(1, n // 2):
        starts = [(at - k) % n * share, (at + k) % n * share]
        outs = scatter_rows(outs, *both([shards[k], shards[n - k]], starts))
    far = (at + n // 2) % n * share
    outs = scatter_rows(outs, *both(list(shards[n // 2]), [far, far + piece // 2]))
    key_weight_grad, value_weight_grad = outs

    over_cols = (((1,), (1,)), ((), ()))
    full = lax.dot_general(key_grad, key_weight, over_cols, preferred_element_type=F32)
    full = full + lax.dot_general(value_grad, value_weight, over_cols, preferred_element_type=F32)
    cols = model // mps
    vision_grad = lax.dynamic_slice_in_dim(full, mp * cols, cols, axis=1)
    for k in range(1, mps):
        sent = lax.dynamic_slice_in_dim(full, (mp + k) % mps * cols, cols, axis=1).astype(BF16)
        vision_grad = vision_grad + lax.ppermute(
            sent, "mp", [(i, (i + k) % mps) for i in range(mps)]
        ).astype(F32)
    vision_grad = vision_grad.astype(BF16).reshape(samples, rows, cols)

    returned = [dq[0]] + [within(dq[r], -r) for r in range(1, samples)]
    query_grad = jnp.stack([lax.select_n((s - x) % samples, *returned) for s in range(samples)])
    return (query_grad, vision_grad, key_weight_grad, value_weight_grad)


def solution(mesh):
    in_specs = (
        P("dp", "seq", "mp"),
        P("dp", "seq", None),
        P(None, "mp"),
        P(None, "mp"),
        P(),
        P(),
        P("dp", "seq", "mp"),
        P("dp"),
    )
    out_specs = (P("dp", "seq", "mp"), P("dp", "seq", "mp"), P(None, "mp"), P(None, "mp"))
    body = functools.partial(local, dict(mesh.shape))
    return jax.shard_map(body, mesh=mesh, in_specs=in_specs, out_specs=out_specs, check_vma=False)
```

```python
import functools
import math

import jax
import jax.numpy as jnp
from jax import lax
from jax.experimental import pallas as pl
from jax.experimental.pallas import tpu as pltpu
from jax.sharding import PartitionSpec as P


MAX_TILES = 4
EPS = 1e-05
NEG = -1e30
F32 = jnp.float32
BF16 = jnp.bfloat16


def attention_kernel(blocks, parts, group, head_dim, me_ref, tiles_ref, gain_ref, *refs):
    q_refs, refs = refs[:parts], refs[parts:]
    g_refs, refs = refs[:parts], refs[parts:]
    kv_refs, refs = refs[:blocks], refs[blocks:]
    dq_refs, refs = refs[:parts], refs[parts:]
    dkv_refs, refs = refs[:blocks], refs[blocks:]
    keys, values, dkeys, dvalues = refs
    dq_refs = [dq_refs[0].at[0]] + list(dq_refs[1:])
    rows = kv_refs[0].shape[0]
    total = rows * blocks
    scale = head_dim ** (-0.5)
    token = lax.broadcasted_iota(jnp.int32, (total, 1), 0)
    live = token < 0
    me = me_ref[0]
    live_end = tiles_ref[lax.rem(me, parts)] * (total // MAX_TILES)
    for k in range(blocks):
        keys[k * rows : (k + 1) * rows, :] = kv_refs[k][:, :head_dim]
        values[k * rows : (k + 1) * rows, :] = kv_refs[k][:, head_dim:]
        start = k * rows
        left = live_end - lax.rem(me + blocks - k, blocks) * rows
        live = live | ((token >= start) & (token < start + jnp.minimum(left, rows)))
    bias = jnp.where(live, 0.0, NEG)
    gain = gain_ref[...]
    keys_all = keys[...]
    values_all = values[...]
    keys_turned = keys_all.T
    values_turned = values_all.T
    over_dims = (((1,), (1,)), ((), ()))

    def front(h):
        cols = slice(h * head_dim, (h + 1) * head_dim)
        raw_b = jnp.concatenate([ref[..., cols].reshape(-1, head_dim) for ref in q_refs], axis=0)
        out_b = jnp.concatenate([ref[..., cols].reshape(-1, head_dim) for ref in g_refs], axis=0)
        raw = raw_b.astype(F32)
        inverse = lax.rsqrt(jnp.mean(raw * raw, axis=-1, keepdims=True) + EPS)
        unit = raw * inverse
        normed = (unit * gain).astype(BF16)
        scores = lax.dot_general(keys_all, normed, over_dims, preferred_element_type=F32)
        dprobs = lax.dot_general(values_all, out_b, over_dims, preferred_element_type=F32)
        return cols, out_b, inverse, unit, normed, scores, dprobs

    def middle(cols, out_b, inverse, unit, normed, scores, dprobs):
        scores = scores * (scale * math.log2(math.e)) + bias
        expo = jnp.exp2(scores - jnp.max(scores, axis=0, keepdims=True))
        probs = expo * (1.0 / jnp.sum(expo, axis=0, keepdims=True))
        probs_b = probs.astype(BF16)
        attn = jnp.dot(values_turned, probs_b, preferred_element_type=F32).astype(BF16)
        delta = jnp.sum(out_b.T.astype(F32) * attn.astype(F32), axis=0, keepdims=True)
        dscores = (probs * (dprobs - delta)).astype(BF16)
        return cols, out_b, inverse, unit, normed, probs_b, dscores

    def back(h, cols, out_b, inverse, unit, normed, probs_b, dscores):
        dnormed = jnp.dot(keys_turned, dscores, preferred_element_type=F32).T * scale
        weighted = dnormed * gain
        grad = inverse * (weighted - unit * jnp.mean(weighted * unit, axis=-1, keepdims=True))
        grad = grad.astype(BF16)
        part_rows = grad.shape[0] // parts
        for p in range(parts):
            dq_refs[p][:, cols] = grad[p * part_rows : (p + 1) * part_rows]
        dk = jnp.dot(dscores, normed, preferred_element_type=F32)
        dv = jnp.dot(probs_b, out_b, preferred_element_type=F32)
        if h == 0:
            dkeys[...] = dk
            dvalues[...] = dv
        else:
            dkeys[...] += dk
            dvalues[...] += dv

    ahead = front(0)
    behind = None
    for h in range(group):
        now = ahead
        if h + 1 < group:
            ahead = front(h + 1)
        mid = middle(*now)
        if behind is not None:
            back(h - 1, *behind)
        behind = mid
    back(group - 1, *behind)
    for k in range(blocks):
        span = slice(k * rows, (k + 1) * rows)
        dkv_refs[k][:, :head_dim] = (dkeys[span, :] * scale).astype(BF16)
        dkv_refs[k][:, head_dim:] = dvalues[span, :].astype(BF16)


def attention(me, tiles, gain, queries, out_grad, others, kv_blocks, head_dim):
    blocks = len(kv_blocks)
    parts = 2
    text_rows, width = queries.shape[1:]
    rows, kv_width = kv_blocks[0].shape
    kv_here = kv_width // (2 * head_dim)
    group = width // head_dim // kv_here
    group_width = group * head_dim
    total = rows * blocks
    own = pl.BlockSpec((1, text_rows, group_width), lambda g, m, t: (lax.rem(m[0], parts), 0, g))
    other = pl.BlockSpec((text_rows, group_width), lambda g, m, t: (0, g))
    below = pl.BlockSpec((text_rows, group_width), lambda g, m, t: (1, g))
    kv = pl.BlockSpec((rows, 2 * head_dim), lambda g, m, t: (0, g))
    gain_spec = pl.BlockSpec((1, head_dim), lambda g, m, t: (0, 0))
    work = text_rows * parts * group * kv_here * total
    results = pl.pallas_call(
        functools.partial(attention_kernel, blocks, parts, group, head_dim),
        grid_spec=pltpu.PrefetchScalarGridSpec(
            num_scalar_prefetch=2,
            grid=(kv_here,),
            in_specs=[gain_spec, own, other, own, below] + [kv] * blocks,
            out_specs=[own, other] + [kv] * blocks,
            scratch_shapes=[pltpu.VMEM((total, head_dim), BF16)] * 2
            + [pltpu.VMEM((total, head_dim), F32)] * 2,
        ),
        out_shape=[jax.ShapeDtypeStruct(queries.shape, BF16), jax.ShapeDtypeStruct((text_rows, width), BF16)]
        + [jax.ShapeDtypeStruct((rows, kv_width), BF16)] * blocks,
        cost_estimate=pl.CostEstimate(
            flops=12 * work * head_dim, bytes_accessed=6 * text_rows * parts * width, transcendentals=work
        ),
        name="attention",
    )(me, tiles, gain.reshape(1, head_dim), queries, others, out_grad, others, *kv_blocks)
    return results[:parts], results[parts:]


def project_kernel(samples, head_dim, me_ref, gain_ref, vision_ref, key_ref, value_ref, *refs):
    raw_ref, kv_refs = refs[0], refs[1 : 1 + samples]
    keys, values = refs[1 + samples :]
    step = pl.program_id(0)
    vision = vision_ref[...]
    key_part = jnp.dot(vision, key_ref[...], preferred_element_type=F32)
    value_part = jnp.dot(vision, value_ref[...], preferred_element_type=F32)

    @pl.when(step == 0)
    def _():
        keys[...] = key_part
        values[...] = value_part

    @pl.when(step > 0)
    def _():
        keys[...] += key_part
        values[...] += value_part

    @pl.when(step == pl.num_programs(0) - 1)
    def _():
        raw_ref[...] = keys[...]
        gain = gain_ref[...]
        rows = kv_refs[0].shape[0]
        x = lax.rem(me_ref[0], samples)
        for r in range(samples):
            start = pl.multiple_of(lax.rem(x + r, samples) * rows, 8)
            for h in range(keys.shape[1] // head_dim):
                cols = slice(h * head_dim, (h + 1) * head_dim)
                raw = keys[pl.ds(start, rows), cols]
                inverse = lax.rsqrt(jnp.mean(raw * raw, axis=-1, keepdims=True) + EPS)
                at = 2 * h * head_dim
                kv_refs[r][:, at : at + head_dim] = (raw * inverse * gain).astype(BF16)
                kv_refs[r][:, at + head_dim : at + 2 * head_dim] = values[pl.ds(start, rows), cols].astype(BF16)


def project(me, gain, vision, key_weight, value_weight, samples):
    all_rows, model = vision.shape
    width = key_weight.shape[1]
    head_dim = gain.shape[0]
    rows = all_rows // samples
    step = math.gcd(model, 512)
    weight = pl.BlockSpec((step, width), lambda i, m: (i, 0))
    results = pl.pallas_call(
        functools.partial(project_kernel, samples, head_dim),
        grid_spec=pltpu.PrefetchScalarGridSpec(
            num_scalar_prefetch=1,
            grid=(model // step,),
            in_specs=[
                pl.BlockSpec((1, head_dim), lambda i, m: (0, 0)),
                pl.BlockSpec((all_rows, step), lambda i, m: (0, i)),
                weight,
                weight,
            ],
            out_specs=[pl.BlockSpec((all_rows, width), lambda i, m: (0, 0))]
            + [pl.BlockSpec((rows, 2 * width), lambda i, m: (0, 0))] * samples,
            scratch_shapes=[pltpu.VMEM((all_rows, width), F32)] * 2,
        ),
        out_shape=[jax.ShapeDtypeStruct((all_rows, width), F32)]
        + [jax.ShapeDtypeStruct((rows, 2 * width), BF16)] * samples,
        cost_estimate=pl.CostEstimate(
            flops=4 * all_rows * model * width,
            bytes_accessed=2 * model * (all_rows + 2 * width),
            transcendentals=0,
        ),
        name="project",
    )(me, gain.reshape(1, head_dim), vision, key_weight, value_weight)
    return results[0], results[1:]


def own_grads_kernel(samples, head_dim, me_ref, gain_ref, raw_ref, *refs):
    arrived, out_ref = refs[:-1], refs[-1]
    rows = arrived[0].shape[0]
    width = raw_ref.shape[1]
    gain = gain_ref[...]
    x = lax.rem(me_ref[0], samples)

    def total(r, cols):
        value = arrived[r][:, cols].astype(F32)
        for k in range(r + samples, len(arrived), samples):
            value = value + arrived[k][:, cols].astype(F32)
        return value

    for r in range(samples):
        start = pl.multiple_of(lax.rem(x + r, samples) * rows, 16)
        for h in range(width // head_dim):
            at = h * head_dim
            raw = raw_ref[pl.ds(start, rows), at : at + head_dim]
            inverse = lax.rsqrt(jnp.mean(raw * raw, axis=-1, keepdims=True) + EPS)
            unit = raw * inverse
            weighted = total(r, slice(2 * at, 2 * at + head_dim)) * gain
            grad = inverse * (weighted - unit * jnp.mean(weighted * unit, axis=-1, keepdims=True))
            out_ref[pl.ds(start, rows), at : at + head_dim] = grad.astype(BF16)
            value = total(r, slice(2 * at + head_dim, 2 * (at + head_dim)))
            out_ref[pl.ds(start, rows), width + at : width + at + head_dim] = value.astype(BF16)


def sum_own_grads(me, gain, key_raw, arrived, samples):
    head_dim = gain.shape[0]
    all_rows, width = key_raw.shape
    whole = pl.BlockSpec(memory_space=pltpu.VMEM)
    return pl.pallas_call(
        functools.partial(own_grads_kernel, samples, head_dim),
        in_specs=[pl.BlockSpec(memory_space=pltpu.SMEM)] + [whole] * (2 + len(arrived)),
        out_specs=whole,
        out_shape=jax.ShapeDtypeStruct((all_rows, 2 * width), BF16),
        cost_estimate=pl.CostEstimate(
            flops=40 * all_rows * width * len(arrived), bytes_accessed=4 * all_rows * width * 5, transcendentals=0
        ),
        name="own_grads",
    )(me, gain.reshape(1, head_dim), key_raw, *arrived)


def weight_kernel(n, dps, samples, where_ref, *refs):
    own_vision, direct, crossed = refs[0], refs[1:n], refs[n]
    refs = refs[n + 1 :]
    grads, refs = refs[: n + 1], refs[n + 1 :]
    keep_ref, sent_refs = refs[0], refs[1:dps]
    vision_all, grads_all = refs[dps:]
    mine, helped = where_ref[0], where_ref[1]
    all_rows = own_vision.shape[0]
    rows = all_rows // samples
    vision_all[:all_rows, :] = own_vision[...]
    for k in range(1, n):
        here = pl.multiple_of(k * all_rows + helped * rows, 16)
        there = pl.multiple_of(k * all_rows + (samples - 1 - helped) * rows, 16)
        vision_all[pl.ds(here, rows), :] = direct[k - 1][...]
        vision_all[pl.ds(there, rows), :] = crossed[(k - 1) * rows : k * rows, :]
    at = 0
    for grad in grads:
        grads_all[at : at + grad.shape[0], :] = grad[...]
        at += grad.shape[0]
    piece = keep_ref.shape[0]
    for r in range(dps):
        cols = pl.ds(pl.multiple_of(lax.rem(mine + r, dps) * piece, 128), piece)
        part = lax.dot_general(
            vision_all[:, cols], grads_all[...], (((0,), (0,)), ((), ())), preferred_element_type=F32
        )
        if r == 0:
            keep_ref[...] = part
        else:
            sent_refs[r - 1][...] = part.astype(BF16)


def weight_grads(where, own_vision, direct, crossed, grads, dps, samples):
    n = 1 + len(direct)
    all_rows, share = own_vision.shape
    width = grads[0].shape[1]
    piece = share // dps
    whole = pl.BlockSpec(memory_space=pltpu.VMEM)
    inputs = [own_vision, *direct, crossed, *grads]
    return pl.pallas_call(
        functools.partial(weight_kernel, n, dps, samples),
        in_specs=[pl.BlockSpec(memory_space=pltpu.SMEM)] + [whole] * len(inputs),
        out_specs=[whole] * dps,
        out_shape=[jax.ShapeDtypeStruct((piece, width), F32)]
        + [jax.ShapeDtypeStruct((piece, width), BF16)] * (dps - 1),
        scratch_shapes=[pltpu.VMEM((n * all_rows, share), BF16), pltpu.VMEM((n * all_rows, width), BF16)],
        cost_estimate=pl.CostEstimate(
            flops=2 * n * all_rows * share * width,
            bytes_accessed=2 * n * all_rows * (share + width),
            transcendentals=0,
        ),
        name="weight_grads",
    )(where, *inputs)


def scatter_kernel(pieces, n, share, where_ref, *refs):
    piece_refs, refs = refs[: len(pieces)], refs[len(pieces) :]
    outs, wide, sem = refs[-4:-2], refs[-2], refs[-1]
    half = outs[0].shape[1]
    at, mine = where_ref[0], where_ref[1]
    copies = []
    top = 0
    for p, (steps, side, core, below) in enumerate(pieces):
        rows = piece_refs[p].shape[0]
        place = lax.rem(at + n + steps + side * mine, n)
        core_at = lax.rem(mine + core, 2)
        start = pl.multiple_of(place * share + core_at * (share // 2) + below, 8)
        for q, out in enumerate(outs):
            wide[q, top : top + rows, :] = piece_refs[p][:, q * half : (q + 1) * half].astype(F32)
            copy = pltpu.make_async_copy(
                wide.at[q, pl.ds(top, rows), :], out.at[pl.ds(start, rows), :], sem.at[p, q]
            )
            copy.start()
            copies.append(copy)
        top += rows
    for copy in copies:
        copy.wait()


def scatter_rows(outs, where, values, pieces, n):
    count = len(values)
    rows = sum(v.shape[0] for v in values)
    width = values[0].shape[1] // 2
    whole = pl.BlockSpec(memory_space=pltpu.VMEM)
    share = outs[0].shape[0] // n
    return pl.pallas_call(
        functools.partial(scatter_kernel, pieces, n, share),
        in_specs=[pl.BlockSpec(memory_space=pltpu.SMEM)]
        + [whole] * count
        + [pl.BlockSpec(memory_space=pl.ANY)] * 2,
        out_specs=[pl.BlockSpec(memory_space=pl.ANY)] * 2,
        scratch_shapes=[pltpu.VMEM((2, rows, width), F32), pltpu.SemaphoreType.DMA((count, 2))],
        out_shape=[jax.ShapeDtypeStruct(o.shape, F32) for o in outs],
        input_output_aliases={1 + count: 0, 2 + count: 1},
        cost_estimate=pl.CostEstimate(flops=rows * width * 2000, bytes_accessed=rows * width * 12, transcendentals=0),
        name="scatter_rows",
    )(where, *values, *outs)


def blank_kernel(*refs):
    pass


def blank(shape):
    return pl.pallas_call(
        blank_kernel,
        out_specs=[pl.BlockSpec(memory_space=pl.ANY)] * 2,
        out_shape=[jax.ShapeDtypeStruct(shape, F32)] * 2,
        name="blank",
    )()


def local(sizes, queries, vision, key_weight, value_weight, query_gain, key_gain, out_grad, tile_count):
    n, dps, mps = sizes["seq"], sizes["dp"], sizes["mp"]
    head_dim = query_gain.shape[0]
    samples, rows, model = vision.shape
    width = key_weight.shape[1]
    me, mine, mp = lax.axis_index("seq"), lax.axis_index("dp"), lax.axis_index("mp")
    x = me % samples
    me_ref = me.astype(jnp.int32).reshape(1)
    order = [i for i in range(0, n, 2)] + [i for i in range(n - 1, 0, -2)]
    at = jnp.where(me % 2 == 0, me // 2, n - 1 - me // 2)
    helped = mp % samples

    def shift(value, k):
        return lax.ppermute(value, "seq", [(i, (i + k) % n) for i in range(n)])

    def ring(value, k):
        return lax.ppermute(value, "seq", [(order[i], order[(i + k) % n]) for i in range(n)])

    def within(value, axis, k, size):
        perm = [(i, i // samples * samples + (i % samples + k) % samples) for i in range(size)]
        return lax.ppermute(value, axis, perm)

    def pick(value, i):
        return lax.dynamic_index_in_dim(value, i % samples, 0, False)

    others = within(jnp.concatenate([pick(queries, x + 1), pick(out_grad, x + 1)], axis=0), "seq", 1, n)

    flat_vision = vision.reshape(samples * rows, model)
    key_raw, kv_rel = project(me_ref, key_gain, flat_vision, key_weight, value_weight, samples)
    kv_blocks = [kv_rel[0]]
    for k in range(1, n):
        kv_blocks.append(shift(kv_rel[k % samples], k))

    share = model // n
    sample_vision = pick(vision, helped)
    direct = []
    for k in range(1, n):
        cut = lax.dynamic_slice_in_dim(sample_vision, (at + k) % n * share, share, axis=1)
        direct.append(ring(cut, k))
    own_vision = lax.dynamic_slice_in_dim(flat_vision, at * share, share, axis=1)

    dq, dkv = attention(
        me_ref, tile_count, query_gain, queries, out_grad, others, kv_blocks, head_dim
    )

    arrived = [dkv[0]]
    for k in range(1, n):
        arrived.append(shift(dkv[k], -k))
    returned = within(dq[1], "seq", 1, n)
    direct = lax.optimization_barrier(direct)
    crossed = within(jnp.concatenate(direct, axis=0), "mp", 1, mps)
    own_grads = sum_own_grads(me_ref, key_gain, key_raw, arrived, samples)

    half = own_grads.shape[0] // 2
    grads = [own_grads] + [None] * n
    up = down = own_grads
    for k in range(1, n // 2):
        up, down = ring(up, 1), ring(down, -1)
        grads[k], grads[n + 1 - k] = up, down
    grads[n // 2], grads[n // 2 + 1] = ring(up[:half], 1), ring(down[half:], -1)
    over_cols = (((1,), (1,)), ((), ()))
    full = lax.dot_general(own_grads[:, :width], key_weight, over_cols, preferred_element_type=F32)
    full = full + lax.dot_general(own_grads[:, width:], value_weight, over_cols, preferred_element_type=F32)
    cols = model // mps
    slices = [lax.dynamic_slice_in_dim(full, (mp + k) % mps * cols, cols, axis=1) for k in range(mps)]
    slices = [slices[0]] + [v.astype(BF16) for v in slices[1:]]
    own_vision, slices = lax.optimization_barrier((own_vision, slices))
    vision_grad = slices[0]
    for k in range(1, mps):
        got = lax.ppermute(slices[k], "mp", [(i, (i + k) % mps) for i in range(mps)])
        vision_grad = vision_grad + got.astype(F32)
    vision_grad = vision_grad.astype(BF16).reshape(samples, rows, cols)

    where = jnp.stack([mine, helped]).astype(jnp.int32)
    keep, sent = weight_grads(where, own_vision, direct, crossed, grads, dps, samples)

    def across(value):
        return lax.ppermute(value, "dp", [(i, (i + 1) % dps) for i in range(dps)])

    def split_ring(value):
        perm = []
        for d in range(dps):
            perm += [(d * n + order[i], d * n + order[(i + 1 - 2 * d) % n]) for i in range(n)]
        return lax.ppermute(value, ("dp", "seq"), perm)

    shard = (keep + across(sent).astype(F32)).astype(BF16)
    spot = jnp.stack([at, mine]).astype(jnp.int32)
    query_grad = lax.dynamic_update_index_in_dim(dq[0], returned, (x + 1) % samples, 0)
    values = [shard, across(shard)]
    outs = blank((model, width))
    outs = scatter_rows(outs, spot, values, ((0, 0, 0, 0), (0, 0, 1, 0)), n)
    far = n // 2
    for k in range(1, far + 1):
        for _ in range(dps if k < far else 1):
            values.append(split_ring(values[-dps]))
        new = values[-dps:] if k < far else values[-1:]
        pieces = tuple((-k, 2 * k, core, 0) for core in range(len(new)))
        pieces += tuple((k, -2 * k, 1 - core, 0) for core in range(len(new)))
        crossing = [across(v) for v in new]
        outs = scatter_rows(outs, spot, list(new) + crossing, pieces, n)
    key_weight_grad, value_weight_grad = outs

    query_grad = lax.dynamic_update_index_in_dim(dq[0], returned, (x + 1) % samples, 0)
    return (query_grad, vision_grad, key_weight_grad, value_weight_grad)


def solution(mesh):
    in_specs = (
        P("dp", "seq", "mp"),
        P("dp", "seq", None),
        P(None, "mp"),
        P(None, "mp"),
        P(),
        P(),
        P("dp", "seq", "mp"),
        P("dp"),
    )
    out_specs = (P("dp", "seq", "mp"), P("dp", "seq", "mp"), P(None, "mp"), P(None, "mp"))

    def body(*args):
        return local(dict(mesh.shape), *args)

    return jax.shard_map(body, mesh=mesh, in_specs=in_specs, out_specs=out_specs, check_vma=False)
```

```python
import functools
import math

import jax
import jax.numpy as jnp
from jax import lax
from jax.experimental import pallas as pl
from jax.experimental.pallas import tpu as pltpu
from jax.sharding import PartitionSpec as P


MAX_TILES = 4
EPS = 1e-05
NEG = -1e30
F32 = jnp.float32
BF16 = jnp.bfloat16


def attention_kernel(blocks, parts, group, head_dim, me_ref, tiles_ref, gain_ref, *refs):
    q_refs, refs = refs[:parts], refs[parts:]
    g_refs, refs = refs[:parts], refs[parts:]
    kv_refs, refs = refs[:blocks], refs[-(parts + blocks + 4) :]
    dq_refs, refs = refs[:parts], refs[parts:]
    dkv_refs, refs = refs[:blocks], refs[blocks:]
    keys, values, dkeys, dvalues = refs
    dq_refs = [dq_refs[0].at[0]] + list(dq_refs[1:])
    rows = kv_refs[0].shape[0]
    total = rows * blocks
    scale = head_dim ** (-0.5)
    token = lax.broadcasted_iota(jnp.int32, (total, 1), 0)
    live = token < 0
    me = me_ref[0]
    live_end = tiles_ref[lax.rem(me, parts)] * (total // MAX_TILES)
    for k in range(blocks):
        keys[k * rows : (k + 1) * rows, :] = kv_refs[k][:, :head_dim]
        values[k * rows : (k + 1) * rows, :] = kv_refs[k][:, head_dim:]
        start = k * rows
        left = live_end - lax.bitwise_xor(me, k) * rows
        live = live | ((token >= start) & (token < start + jnp.minimum(left, rows)))
    bias = jnp.where(live, 0.0, NEG)
    gain = gain_ref[...]
    keys_all = keys[...]
    values_all = values[...]
    keys_turned = keys_all.T
    values_turned = values_all.T
    over_dims = (((1,), (1,)), ((), ()))

    def front(h):
        cols = slice(h * head_dim, (h + 1) * head_dim)
        raw_b = jnp.concatenate([ref[..., cols].reshape(-1, head_dim) for ref in q_refs], axis=0)
        out_b = jnp.concatenate([ref[..., cols].reshape(-1, head_dim) for ref in g_refs], axis=0)
        raw = raw_b.astype(F32)
        inverse = lax.rsqrt(jnp.mean(raw * raw, axis=-1, keepdims=True) + EPS)
        unit = raw * inverse
        normed = (unit * gain).astype(BF16)
        scores = lax.dot_general(keys_all, normed, over_dims, preferred_element_type=F32)
        dprobs = lax.dot_general(values_all, out_b, over_dims, preferred_element_type=F32)
        return cols, out_b, inverse, unit, normed, scores, dprobs

    def middle(cols, out_b, inverse, unit, normed, scores, dprobs):
        scores = scores * (scale * math.log2(math.e)) + bias
        expo = jnp.exp2(scores - jnp.max(scores, axis=0, keepdims=True))
        probs = expo * (1.0 / jnp.sum(expo, axis=0, keepdims=True))
        probs_b = probs.astype(BF16)
        attn = jnp.dot(values_turned, probs_b, preferred_element_type=F32).astype(BF16)
        delta = jnp.sum(out_b.T.astype(F32) * attn.astype(F32), axis=0, keepdims=True)
        dscores = (probs * (dprobs - delta)).astype(BF16)
        return cols, out_b, inverse, unit, normed, probs_b, dscores

    def back(h, cols, out_b, inverse, unit, normed, probs_b, dscores):
        dnormed = jnp.dot(keys_turned, dscores, preferred_element_type=F32).T * scale
        weighted = dnormed * gain
        grad = inverse * (weighted - unit * jnp.mean(weighted * unit, axis=-1, keepdims=True))
        grad = grad.astype(BF16)
        part_rows = grad.shape[0] // parts
        for p in range(parts):
            dq_refs[p][:, cols] = grad[p * part_rows : (p + 1) * part_rows]
        dk = jnp.dot(dscores, normed, preferred_element_type=F32)
        dv = jnp.dot(probs_b, out_b, preferred_element_type=F32)
        if h == 0:
            dkeys[...] = dk
            dvalues[...] = dv
        else:
            dkeys[...] += dk
            dvalues[...] += dv

    ahead = front(0)
    behind = None
    for h in range(group):
        now = ahead
        if h + 1 < group:
            ahead = front(h + 1)
        mid = middle(*now)
        if behind is not None:
            back(h - 1, *behind)
        behind = mid
    back(group - 1, *behind)
    for k in range(blocks):
        span = slice(k * rows, (k + 1) * rows)
        dkv_refs[k][:, :head_dim] = (dkeys[span, :] * scale).astype(BF16)
        dkv_refs[k][:, head_dim:] = dvalues[span, :].astype(BF16)


def attention(me, tiles, gain, queries, out_grad, others, kv_blocks, head_dim, kv_here, first, before):
    blocks = len(kv_blocks)
    parts = 2
    text_rows, width = queries.shape[1:]
    rows, kv_width = kv_blocks[0].shape
    heads = kv_width // (2 * head_dim)
    group = width // head_dim // kv_here
    group_width = group * head_dim
    total = rows * blocks
    own = pl.BlockSpec((1, text_rows, group_width), lambda g, m, t: (lax.rem(m[0], parts), 0, g + first))
    other = pl.BlockSpec((text_rows, group_width), lambda g, m, t: (0, g + first))
    below = pl.BlockSpec((text_rows, group_width), lambda g, m, t: (1, g + first))
    kv = pl.BlockSpec((rows, 2 * head_dim), lambda g, m, t: (0, g))
    dkv = pl.BlockSpec((rows, 2 * head_dim), lambda g, m, t: (0, g + first))
    gain_spec = pl.BlockSpec((1, head_dim), lambda g, m, t: (0, 0))
    work = text_rows * parts * group * heads * total
    results = pl.pallas_call(
        functools.partial(attention_kernel, blocks, parts, group, head_dim),
        grid_spec=pltpu.PrefetchScalarGridSpec(
            num_scalar_prefetch=2,
            grid=(heads,),
            in_specs=[gain_spec, own, other, own, below]
            + [kv] * blocks
            + [pl.BlockSpec(memory_space=pl.ANY)] * len(before),
            out_specs=[own, other] + [dkv] * blocks,
            scratch_shapes=[pltpu.VMEM((total, head_dim), BF16)] * 2
            + [pltpu.VMEM((total, head_dim), F32)] * 2,
        ),
        out_shape=[jax.ShapeDtypeStruct(queries.shape, BF16), jax.ShapeDtypeStruct((text_rows, width), BF16)]
        + [jax.ShapeDtypeStruct((rows, 2 * head_dim * kv_here), BF16)] * blocks,
        input_output_aliases={7 + blocks + i: i for i in range(len(before))},
        cost_estimate=pl.CostEstimate(
            flops=12 * work * head_dim,
            bytes_accessed=6 * text_rows * parts * group_width * heads,
            transcendentals=work,
        ),
        name="attention",
    )(me, tiles, gain.reshape(1, head_dim), queries, others, out_grad, others, *kv_blocks, *before)
    return results


def project_kernel(samples, chunks, head_dim, me_ref, gain_ref, vision_ref, key_ref, value_ref, *refs):
    raw_ref, kv_refs, (keys, values) = refs[0], refs[1:-2], refs[-2:]
    step = pl.program_id(0)
    vision = vision_ref[...]
    key_part = jnp.dot(vision, key_ref[...], preferred_element_type=F32)
    value_part = jnp.dot(vision, value_ref[...], preferred_element_type=F32)

    @pl.when(step == 0)
    def _():
        keys[...] = key_part
        values[...] = value_part

    @pl.when(step > 0)
    def _():
        keys[...] += key_part
        values[...] += value_part

    @pl.when(step == pl.num_programs(0) - 1)
    def _():
        raw_ref[...] = keys[...]
        gain = gain_ref[...]
        rows = kv_refs[0].shape[0]
        x = lax.rem(me_ref[0], samples)
        for r in range(samples):
            start = pl.multiple_of(lax.rem(x + r, samples) * rows, 8)
            heads = keys.shape[1] // head_dim
            for h in range(heads):
                cols = slice(h * head_dim, (h + 1) * head_dim)
                raw = keys[pl.ds(start, rows), cols]
                inverse = lax.rsqrt(jnp.mean(raw * raw, axis=-1, keepdims=True) + EPS)
                kv_ref = kv_refs[r * chunks + h * chunks // heads]
                at = 2 * (h % (heads // chunks)) * head_dim
                kv_ref[:, at : at + head_dim] = (raw * inverse * gain).astype(BF16)
                kv_ref[:, at + head_dim : at + 2 * head_dim] = values[pl.ds(start, rows), cols].astype(BF16)


def project(me, gain, vision, key_weight, value_weight, samples, chunks):
    all_rows, model = vision.shape
    width = key_weight.shape[1]
    head_dim = gain.shape[0]
    rows = all_rows // samples
    step = math.gcd(model, 512)
    weight = pl.BlockSpec((step, width), lambda i, m: (i, 0))
    results = pl.pallas_call(
        functools.partial(project_kernel, samples, chunks, head_dim),
        grid_spec=pltpu.PrefetchScalarGridSpec(
            num_scalar_prefetch=1,
            grid=(model // step,),
            in_specs=[
                pl.BlockSpec((1, head_dim), lambda i, m: (0, 0)),
                pl.BlockSpec((all_rows, step), lambda i, m: (0, i)),
                weight,
                weight,
            ],
            out_specs=[pl.BlockSpec((all_rows, width), lambda i, m: (0, 0))]
            + [pl.BlockSpec((rows, 2 * width // chunks), lambda i, m: (0, 0))] * (samples * chunks),
            scratch_shapes=[pltpu.VMEM((all_rows, width), F32)] * 2,
        ),
        out_shape=[jax.ShapeDtypeStruct((all_rows, width), F32)]
        + [jax.ShapeDtypeStruct((rows, 2 * width // chunks), BF16)] * (samples * chunks),
        cost_estimate=pl.CostEstimate(
            flops=4 * all_rows * model * width,
            bytes_accessed=2 * model * (all_rows + 2 * width),
            transcendentals=0,
        ),
        name="project",
    )(me, gain.reshape(1, head_dim), vision, key_weight, value_weight)
    return results[0], [results[1 + r * chunks : 1 + (r + 1) * chunks] for r in range(samples)]


def own_grads_kernel(samples, head_dim, me_ref, gain_ref, raw_ref, *refs):
    arrived, out_ref = refs[:-1], refs[-1]
    rows = arrived[0].shape[0]
    width = raw_ref.shape[1]
    gain = gain_ref[...]
    x = lax.rem(me_ref[0], samples)

    def total(r, cols):
        value = arrived[r][:, cols].astype(F32)
        for k in range(r + samples, len(arrived), samples):
            value = value + arrived[k][:, cols].astype(F32)
        return value

    for r in range(samples):
        start = pl.multiple_of(lax.rem(x + r, samples) * rows, 16)
        for h in range(width // head_dim):
            at = h * head_dim
            raw = raw_ref[pl.ds(start, rows), at : at + head_dim]
            inverse = lax.rsqrt(jnp.mean(raw * raw, axis=-1, keepdims=True) + EPS)
            unit = raw * inverse
            weighted = total(r, slice(2 * at, 2 * at + head_dim)) * gain
            grad = inverse * (weighted - unit * jnp.mean(weighted * unit, axis=-1, keepdims=True))
            out_ref[pl.ds(start, rows), at : at + head_dim] = grad.astype(BF16)
            value = total(r, slice(2 * at + head_dim, 2 * (at + head_dim)))
            out_ref[pl.ds(start, rows), width + at : width + at + head_dim] = value.astype(BF16)


def sum_own_grads(me, gain, key_raw, arrived, samples):
    head_dim = gain.shape[0]
    all_rows, width = key_raw.shape
    whole = pl.BlockSpec(memory_space=pltpu.VMEM)
    return pl.pallas_call(
        functools.partial(own_grads_kernel, samples, head_dim),
        in_specs=[pl.BlockSpec(memory_space=pltpu.SMEM)] + [whole] * (2 + len(arrived)),
        out_specs=whole,
        out_shape=jax.ShapeDtypeStruct((all_rows, 2 * width), BF16),
        cost_estimate=pl.CostEstimate(
            flops=40 * all_rows * width * len(arrived), bytes_accessed=4 * all_rows * width * 5, transcendentals=0
        ),
        name="own_grads",
    )(me, gain.reshape(1, head_dim), key_raw, *arrived)


def pack_kernel(samples, where_ref, *refs):
    blocks, (stay_ref, go_ref) = refs[:-2], refs[-2:]
    x = lax.rem(where_ref[2], samples)
    rows, share = blocks[0].shape[0], stay_ref.shape[1]
    for z, block in enumerate(blocks):
        span = slice(z * rows, (z + 1) * rows)
        stay_ref[span, :] = block[:, pl.ds(pl.multiple_of(x * share, 128), share)]
        go_ref[span, :] = block[:, pl.ds(pl.multiple_of((samples - 1 - x) * share, 128), share)]


def pack(where, blocks, samples):
    rows, width = blocks[0].shape
    whole = pl.BlockSpec(memory_space=pltpu.VMEM)
    shape = jax.ShapeDtypeStruct((len(blocks) * rows, width // samples), BF16)
    return pl.pallas_call(
        functools.partial(pack_kernel, samples),
        in_specs=[pl.BlockSpec(memory_space=pltpu.SMEM)] + [whole] * len(blocks),
        out_specs=[whole] * 2,
        out_shape=[shape] * 2,
        cost_estimate=pl.CostEstimate(
            flops=0, bytes_accessed=4 * len(blocks) * rows * width, transcendentals=0
        ),
        name="pack",
    )(where, *blocks)


def weight_kernel(n, dps, samples, where_ref, *refs):
    vision, grads, refs = refs[:4], refs[4 : n + 4], refs[n + 4 :]
    keep_ref, sent_refs = refs[0], refs[1:dps]
    vision_all, grads_all = refs[dps:]
    mine, helped, me = where_ref[0], where_ref[1], where_ref[2]
    rows = vision[0].shape[0] * samples // n
    all_rows = rows * samples

    def place_of(i):
        return jnp.where(lax.rem(i, 2) == 0, lax.div(i, 2), n - 1 - lax.div(i, 2))

    for j in range(n):
        k = lax.rem(place_of(me) + n - place_of(lax.bitwise_xor(me, j)), n)
        span = slice(j // 2 * rows, (j // 2 + 1) * rows)
        here = pl.multiple_of(k * all_rows + helped * rows, 16)
        there = pl.multiple_of(k * all_rows + (samples - 1 - helped) * rows, 16)
        vision_all[pl.ds(here, rows), :] = vision[j % 2][span, :]
        vision_all[pl.ds(there, rows), :] = vision[2 + j % 2][span, :]
    for k in range(n):
        place = jnp.where(mine == 0, k, (n - k) % n)
        grads_all[pl.ds(pl.multiple_of(place * all_rows, 16), all_rows), :] = grads[k][...]
    piece = keep_ref.shape[0]
    for r in range(dps):
        cols = pl.ds(pl.multiple_of(lax.rem(mine + r, dps) * piece, 128), piece)
        part = lax.dot_general(
            vision_all[:, cols], grads_all[...], (((0,), (0,)), ((), ())), preferred_element_type=F32
        )
        if r == 0:
            keep_ref[...] = part
        else:
            sent_refs[r - 1][...] = part.astype(BF16)


def weight_grads(where, vision, grads, n, dps, samples):
    share = vision[0].shape[1]
    all_rows = vision[0].shape[0] * samples * samples // n
    width = grads[0].shape[1]
    piece = share // dps
    whole = pl.BlockSpec(memory_space=pltpu.VMEM)
    inputs = [*vision, *grads]
    return pl.pallas_call(
        functools.partial(weight_kernel, n, dps, samples),
        in_specs=[pl.BlockSpec(memory_space=pltpu.SMEM)] + [whole] * len(inputs),
        out_specs=[whole] * dps,
        out_shape=[jax.ShapeDtypeStruct((piece, width), F32)]
        + [jax.ShapeDtypeStruct((piece, width), BF16)] * (dps - 1),
        scratch_shapes=[pltpu.VMEM((n * all_rows, share), BF16), pltpu.VMEM((n * all_rows, width), BF16)],
        cost_estimate=pl.CostEstimate(
            flops=2 * n * all_rows * share * width,
            bytes_accessed=2 * n * all_rows * (share + width),
            transcendentals=0,
        ),
        name="weight_grads",
    )(where, *inputs)


def scatter_kernel(pieces, n, share, where_ref, *refs):
    piece_refs, refs = refs[: len(pieces)], refs[len(pieces) :]
    outs, wide, sem = refs[-4:-2], refs[-2], refs[-1]
    half = outs[0].shape[1]
    at, mine = where_ref[0], where_ref[1]
    copies = []
    top = 0
    for p, (steps, side, core, below) in enumerate(pieces):
        rows = piece_refs[p].shape[0]
        place = lax.rem(at + n + steps + side * mine, n)
        core_at = lax.rem(mine + core, 2)
        device = jnp.where(place < n // 2, 2 * place, 2 * (n - 1 - place) + 1)
        start = pl.multiple_of(device * share + core_at * (share // 2) + below, 8)
        for q, out in enumerate(outs):
            wide[q, top : top + rows, :] = piece_refs[p][:, q * half : (q + 1) * half].astype(F32)
            copy = pltpu.make_async_copy(
                wide.at[q, pl.ds(top, rows), :], out.at[pl.ds(start, rows), :], sem.at[p, q]
            )
            copy.start()
            copies.append(copy)
        top += rows
    for copy in copies:
        copy.wait()


def scatter_rows(outs, where, values, pieces, n):
    count = len(values)
    rows = sum(v.shape[0] for v in values)
    width = values[0].shape[1] // 2
    whole = pl.BlockSpec(memory_space=pltpu.VMEM)
    share = outs[0].shape[0] // n
    return pl.pallas_call(
        functools.partial(scatter_kernel, pieces, n, share),
        in_specs=[pl.BlockSpec(memory_space=pltpu.SMEM)]
        + [whole] * count
        + [pl.BlockSpec(memory_space=pl.ANY)] * 2,
        out_specs=[pl.BlockSpec(memory_space=pl.ANY)] * 2,
        scratch_shapes=[pltpu.VMEM((2, rows, width), F32), pltpu.SemaphoreType.DMA((count, 2))],
        out_shape=[jax.ShapeDtypeStruct(o.shape, F32) for o in outs],
        input_output_aliases={1 + count: 0, 2 + count: 1},
        cost_estimate=pl.CostEstimate(flops=rows * width * 2000, bytes_accessed=rows * width * 12, transcendentals=0),
        name="scatter_rows",
    )(where, *values, *outs)


def blank_kernel(*refs):
    pass


def blank(shape):
    return pl.pallas_call(
        blank_kernel,
        out_specs=[pl.BlockSpec(memory_space=pl.ANY)] * 2,
        out_shape=[jax.ShapeDtypeStruct(shape, F32)] * 2,
        name="blank",
    )()


def local(sizes, queries, vision, key_weight, value_weight, query_gain, key_gain, out_grad, tile_count):
    n, dps, mps = sizes["seq"], sizes["dp"], sizes["mp"]
    head_dim = query_gain.shape[0]
    samples, rows, model = vision.shape
    width = key_weight.shape[1]
    me, mine, mp = lax.axis_index("seq"), lax.axis_index("dp"), lax.axis_index("mp")
    x = me % samples
    me_ref = me.astype(jnp.int32).reshape(1)
    order = [i for i in range(0, n, 2)] + [i for i in range(n - 1, 0, -2)]
    helped = mp % samples

    assert n & (n - 1) == 0 and samples == 2
    far_first = sorted(range(1, n), key=lambda j: (-((j // 2).bit_length()), -(j // 2), j % 2))

    def swap(value, j):
        return lax.ppermute(value, "seq", [(i, i ^ j) for i in range(n)])

    def place_of(i):
        return jnp.where(i % 2 == 0, i // 2, n - 1 - i // 2)

    def within(value, axis, k, size):
        perm = [(i, i // samples * samples + (i % samples + k) % samples) for i in range(size)]
        return lax.ppermute(value, axis, perm)

    def pick(value, i):
        return lax.dynamic_index_in_dim(value, i % samples, 0, False)

    flat_vision = vision.reshape(samples * rows, model)
    kv_here = width // head_dim
    chunks = chunks_of(kv_here)
    key_raw, kv_rel = project(me_ref, key_gain, flat_vision, key_weight, value_weight, samples, chunks)
    kv_blocks = []
    for c in range(chunks):
        pair = swap(kv_rel[1][c], 1)
        blocks = [kv_rel[0][c], pair] + [None] * (n - 2)
        for z in range(n // 2 - 1, 0, -1):
            blocks[2 * z] = swap(kv_rel[0][c], 2 * z)
            blocks[2 * z + 1] = swap(pair, 2 * z)
        kv_blocks.append(blocks)

    others = swap(jnp.concatenate([pick(queries, x + 1), pick(out_grad, x + 1)], axis=0), 1)

    share = model // n
    at = place_of(me)
    where = jnp.stack([mine, helped, me]).astype(jnp.int32)
    sample_vision = pick(vision, helped)

    def cut(z):
        return lax.dynamic_slice_in_dim(sample_vision, z * samples * share, samples * share, axis=1)

    lines = [cut(me // 2)] + [None] * (n // 2 - 1)
    for z in range(n // 2 - 1, 0, -1):
        lines[z] = swap(cut(me // 2 ^ z), 2 * z)

    results = []
    for c in range(chunks):
        results = attention(
            me_ref, tile_count, query_gain, queries, out_grad, others, kv_blocks[c], head_dim,
            kv_here, c * kv_here // chunks, results,
        )
    dq, dkv = results[:2], results[2:]

    arrived = [dkv[0]] + [None] * (n - 1)
    for j in far_first:
        arrived[j] = swap(dkv[j], j)
    returned = within(dq[1], "seq", 1, n)
    vision_near, going = pack(where, lines, samples)
    vision_far = swap(going, 1)
    cross_near = within(vision_near, "mp", 1, mps)
    cross_far = within(vision_far, "mp", 1, mps)
    vision_rows = [vision_near, vision_far, cross_near, cross_far]
    own_grads = sum_own_grads(me_ref, key_gain, key_raw, arrived, samples)

    def across(value):
        return lax.ppermute(value, "dp", [(i, (i + 1) % dps) for i in range(dps)])

    def split_ring(value):
        perm = []
        for d in range(dps):
            perm += [(d * n + order[i], d * n + order[(i + 1 - 2 * d) % n]) for i in range(n)]
        return lax.ppermute(value, ("dp", "seq"), perm)

    grads = [own_grads] + [None] * (n - 1)
    held = [own_grads, across(own_grads)]
    for k in range(1, n // 2):
        held = [split_ring(v) for v in held]
        grads[k], grads[n - k] = held[0], across(held[1])
    grads[n // 2] = split_ring(held[0])

    over_cols = (((1,), (1,)), ((), ()))
    full = lax.dot_general(own_grads[:, :width], key_weight, over_cols, preferred_element_type=F32)
    full = full + lax.dot_general(own_grads[:, width:], value_weight, over_cols, preferred_element_type=F32)
    cols = model // mps
    slices = [lax.dynamic_slice_in_dim(full, (mp + k) % mps * cols, cols, axis=1) for k in range(mps)]
    slices = [slices[0]] + [v.astype(BF16) for v in slices[1:]]
    vision_rows, slices = lax.optimization_barrier((vision_rows, slices))
    received = []
    for k in range(1, mps):
        received.append(lax.ppermute(slices[k], "mp", [(i, (i + k) % mps) for i in range(mps)]))
    vision_grad = slices[0]
    for got in received:
        vision_grad = vision_grad + got.astype(F32)
    vision_grad = vision_grad.astype(BF16).reshape(samples, rows, cols)

    keep, sent = weight_grads(where, vision_rows, grads, n, dps, samples)

    shard = (keep + across(sent).astype(F32)).astype(BF16)
    spot = jnp.stack([at, mine]).astype(jnp.int32)
    query_grad = lax.dynamic_update_index_in_dim(dq[0], returned, (x + 1) % samples, 0)
    values = [shard, across(shard)]
    outs = blank((model, width))
    outs = scatter_rows(outs, spot, values, ((0, 0, 0, 0), (0, 0, 1, 0)), n)
    far = n // 2
    for k in range(1, far + 1):
        for _ in range(dps if k < far else 1):
            values.append(split_ring(values[-dps]))
        new = values[-dps:] if k < far else values[-1:]
        pieces = tuple((-k, 2 * k, core, 0) for core in range(len(new)))
        pieces += tuple((k, -2 * k, 1 - core, 0) for core in range(len(new)))
        crossing = [across(v) for v in new]
        outs = scatter_rows(outs, spot, list(new) + crossing, pieces, n)
    key_weight_grad, value_weight_grad = outs

    query_grad = lax.dynamic_update_index_in_dim(dq[0], returned, (x + 1) % samples, 0)
    return (query_grad, vision_grad, key_weight_grad, value_weight_grad)


def chunks_of(kv_here):
    return 2 if kv_here % 2 == 0 else 1


def solution(mesh):
    in_specs = (
        P("dp", "seq", "mp"),
        P("dp", "seq", None),
        P(None, "mp"),
        P(None, "mp"),
        P(),
        P(),
        P("dp", "seq", "mp"),
        P("dp"),
    )
    out_specs = (P("dp", "seq", "mp"), P("dp", "seq", "mp"), P(None, "mp"), P(None, "mp"))

    def body(*args):
        return local(dict(mesh.shape), *args)

    step = jax.shard_map(body, mesh=mesh, in_specs=in_specs, out_specs=out_specs, check_vma=False)
    return lambda *args: step(*args)
```

```python
import functools
import math

import jax
import jax.numpy as jnp
from jax import lax
from jax.experimental import pallas as pl
from jax.experimental.pallas import tpu as pltpu
from jax.sharding import PartitionSpec as P


MAX_TILES = 4
EPS = 1e-05
NEG = -1e30
F32 = jnp.float32
BF16 = jnp.bfloat16


def attention_kernel(blocks, parts, group, head_dim, me_ref, tiles_ref, gain_ref, *refs):
    q_refs, refs = refs[:parts], refs[parts:]
    g_refs, refs = refs[:parts], refs[parts:]
    kv_refs, refs = refs[:blocks], refs[-(parts + blocks + 4) :]
    dq_refs, refs = refs[:parts], refs[parts:]
    dkv_refs, refs = refs[:blocks], refs[blocks:]
    keys, values, dkeys, dvalues = refs
    dq_refs = [dq_refs[0].at[0]] + list(dq_refs[1:])
    rows = kv_refs[0].shape[0]
    total = rows * blocks
    scale = head_dim ** (-0.5)
    token = lax.broadcasted_iota(jnp.int32, (total, 1), 0)
    live = token < 0
    me = me_ref[0]
    live_end = tiles_ref[lax.rem(me, parts)] * (total // MAX_TILES)
    for k in range(blocks):
        keys[k * rows : (k + 1) * rows, :] = kv_refs[k][:, :head_dim]
        values[k * rows : (k + 1) * rows, :] = kv_refs[k][:, head_dim:]
        start = k * rows
        left = live_end - lax.bitwise_xor(me, k) * rows
        live = live | ((token >= start) & (token < start + jnp.minimum(left, rows)))
    bias = jnp.where(live, 0.0, NEG)
    gain = gain_ref[...]
    keys_all = keys[...]
    values_all = values[...]
    keys_turned = keys_all.T
    values_turned = values_all.T
    over_dims = (((1,), (1,)), ((), ()))

    def front(h):
        cols = slice(h * head_dim, (h + 1) * head_dim)
        raw_b = jnp.concatenate([ref[..., cols].reshape(-1, head_dim) for ref in q_refs], axis=0)
        out_b = jnp.concatenate([ref[..., cols].reshape(-1, head_dim) for ref in g_refs], axis=0)
        raw = raw_b.astype(F32)
        inverse = lax.rsqrt(jnp.mean(raw * raw, axis=-1, keepdims=True) + EPS)
        unit = raw * inverse
        normed = (unit * gain).astype(BF16)
        scores = lax.dot_general(keys_all, normed, over_dims, preferred_element_type=F32)
        dprobs = lax.dot_general(values_all, out_b, over_dims, preferred_element_type=F32)
        return cols, out_b, inverse, unit, normed, scores, dprobs

    def middle(cols, out_b, inverse, unit, normed, scores, dprobs):
        scores = scores * (scale * math.log2(math.e)) + bias
        expo = jnp.exp2(scores - jnp.max(scores, axis=0, keepdims=True))
        probs = expo * (1.0 / jnp.sum(expo, axis=0, keepdims=True))
        probs_b = probs.astype(BF16)
        attn = jnp.dot(values_turned, probs_b, preferred_element_type=F32).astype(BF16)
        delta = jnp.sum(out_b.T.astype(F32) * attn.astype(F32), axis=0, keepdims=True)
        dscores = (probs * (dprobs - delta)).astype(BF16)
        return cols, out_b, inverse, unit, normed, probs_b, dscores

    def back(h, cols, out_b, inverse, unit, normed, probs_b, dscores):
        dnormed = jnp.dot(keys_turned, dscores, preferred_element_type=F32).T * scale
        weighted = dnormed * gain
        grad = inverse * (weighted - unit * jnp.mean(weighted * unit, axis=-1, keepdims=True))
        grad = grad.astype(BF16)
        part_rows = grad.shape[0] // parts
        for p in range(parts):
            dq_refs[p][:, cols] = grad[p * part_rows : (p + 1) * part_rows]
        dk = jnp.dot(dscores, normed, preferred_element_type=F32)
        dv = jnp.dot(probs_b, out_b, preferred_element_type=F32)
        if h == 0:
            dkeys[...] = dk
            dvalues[...] = dv
        else:
            dkeys[...] += dk
            dvalues[...] += dv

    ahead = front(0)
    behind = None
    for h in range(group):
        now = ahead
        if h + 1 < group:
            ahead = front(h + 1)
        mid = middle(*now)
        if behind is not None:
            back(h - 1, *behind)
        behind = mid
    back(group - 1, *behind)
    for k in range(blocks):
        span = slice(k * rows, (k + 1) * rows)
        dkv_refs[k][:, :head_dim] = (dkeys[span, :] * scale).astype(BF16)
        dkv_refs[k][:, head_dim:] = dvalues[span, :].astype(BF16)


def attention(me, tiles, gain, queries, out_grad, others, kv_blocks, head_dim, kv_here, first, before):
    blocks = len(kv_blocks)
    parts = 2
    text_rows, width = queries.shape[1:]
    rows, kv_width = kv_blocks[0].shape
    heads = kv_width // (2 * head_dim)
    group = width // head_dim // kv_here
    group_width = group * head_dim
    total = rows * blocks
    own = pl.BlockSpec((1, text_rows, group_width), lambda g, m, t: (lax.rem(m[0], parts), 0, g + first))
    other = pl.BlockSpec((text_rows, group_width), lambda g, m, t: (0, g + first))
    below = pl.BlockSpec((text_rows, group_width), lambda g, m, t: (1, g + first))
    kv = pl.BlockSpec((rows, 2 * head_dim), lambda g, m, t: (0, g))
    dkv = pl.BlockSpec((rows, 2 * head_dim), lambda g, m, t: (0, g + first))
    gain_spec = pl.BlockSpec((1, head_dim), lambda g, m, t: (0, 0))
    work = text_rows * parts * group * heads * total
    results = pl.pallas_call(
        functools.partial(attention_kernel, blocks, parts, group, head_dim),
        grid_spec=pltpu.PrefetchScalarGridSpec(
            num_scalar_prefetch=2,
            grid=(heads,),
            in_specs=[gain_spec, own, other, own, below]
            + [kv] * blocks
            + [pl.BlockSpec(memory_space=pl.ANY)] * len(before),
            out_specs=[own, other] + [dkv] * blocks,
            scratch_shapes=[pltpu.VMEM((total, head_dim), BF16)] * 2
            + [pltpu.VMEM((total, head_dim), F32)] * 2,
        ),
        out_shape=[jax.ShapeDtypeStruct(queries.shape, BF16), jax.ShapeDtypeStruct((text_rows, width), BF16)]
        + [jax.ShapeDtypeStruct((rows, 2 * head_dim * kv_here), BF16)] * blocks,
        input_output_aliases={7 + blocks + i: i for i in range(len(before))},
        cost_estimate=pl.CostEstimate(
            flops=12 * work * head_dim,
            bytes_accessed=6 * text_rows * parts * group_width * heads,
            transcendentals=work,
        ),
        name="attention",
    )(me, tiles, gain.reshape(1, head_dim), queries, others, out_grad, others, *kv_blocks, *before)
    return results


def project_kernel(samples, chunks, head_dim, me_ref, gain_ref, vision_ref, key_ref, value_ref, *refs):
    raw_ref, kv_refs, (keys, values) = refs[0], refs[1:-2], refs[-2:]
    step = pl.program_id(0)
    vision = vision_ref[...]
    key_part = jnp.dot(vision, key_ref[...], preferred_element_type=F32)
    value_part = jnp.dot(vision, value_ref[...], preferred_element_type=F32)

    @pl.when(step == 0)
    def _():
        keys[...] = key_part
        values[...] = value_part

    @pl.when(step > 0)
    def _():
        keys[...] += key_part
        values[...] += value_part

    @pl.when(step == pl.num_programs(0) - 1)
    def _():
        raw_ref[...] = keys[...]
        gain = gain_ref[...]
        rows = kv_refs[0].shape[0]
        x = lax.rem(me_ref[0], samples)
        for r in range(samples):
            start = pl.multiple_of(lax.rem(x + r, samples) * rows, 8)
            heads = keys.shape[1] // head_dim
            for h in range(heads):
                cols = slice(h * head_dim, (h + 1) * head_dim)
                raw = keys[pl.ds(start, rows), cols]
                inverse = lax.rsqrt(jnp.mean(raw * raw, axis=-1, keepdims=True) + EPS)
                kv_ref = kv_refs[r * chunks + h * chunks // heads]
                at = 2 * (h % (heads // chunks)) * head_dim
                kv_ref[:, at : at + head_dim] = (raw * inverse * gain).astype(BF16)
                kv_ref[:, at + head_dim : at + 2 * head_dim] = values[pl.ds(start, rows), cols].astype(BF16)


def project(me, gain, vision, key_weight, value_weight, samples, chunks):
    all_rows, model = vision.shape
    width = key_weight.shape[1]
    head_dim = gain.shape[0]
    rows = all_rows // samples
    step = math.gcd(model, 512)
    weight = pl.BlockSpec((step, width), lambda i, m: (i, 0))
    results = pl.pallas_call(
        functools.partial(project_kernel, samples, chunks, head_dim),
        grid_spec=pltpu.PrefetchScalarGridSpec(
            num_scalar_prefetch=1,
            grid=(model // step,),
            in_specs=[
                pl.BlockSpec((1, head_dim), lambda i, m: (0, 0)),
                pl.BlockSpec((all_rows, step), lambda i, m: (0, i)),
                weight,
                weight,
            ],
            out_specs=[pl.BlockSpec((all_rows, width), lambda i, m: (0, 0))]
            + [pl.BlockSpec((rows, 2 * width // chunks), lambda i, m: (0, 0))] * (samples * chunks),
            scratch_shapes=[pltpu.VMEM((all_rows, width), F32)] * 2,
        ),
        out_shape=[jax.ShapeDtypeStruct((all_rows, width), F32)]
        + [jax.ShapeDtypeStruct((rows, 2 * width // chunks), BF16)] * (samples * chunks),
        cost_estimate=pl.CostEstimate(
            flops=4 * all_rows * model * width,
            bytes_accessed=2 * model * (all_rows + 2 * width),
            transcendentals=0,
        ),
        name="project",
    )(me, gain.reshape(1, head_dim), vision, key_weight, value_weight)
    return results[0], [results[1 + r * chunks : 1 + (r + 1) * chunks] for r in range(samples)]


def own_grads_kernel(samples, head_dim, me_ref, gain_ref, raw_ref, *refs):
    arrived, out_ref = refs[:-1], refs[-1]
    rows = arrived[0].shape[0]
    width = raw_ref.shape[1]
    gain = gain_ref[...]
    x = lax.rem(me_ref[0], samples)

    def total(r, cols):
        value = arrived[r][:, cols].astype(F32)
        for k in range(r + samples, len(arrived), samples):
            value = value + arrived[k][:, cols].astype(F32)
        return value

    for r in range(samples):
        start = pl.multiple_of(lax.rem(x + r, samples) * rows, 16)
        for h in range(width // head_dim):
            at = h * head_dim
            raw = raw_ref[pl.ds(start, rows), at : at + head_dim]
            inverse = lax.rsqrt(jnp.mean(raw * raw, axis=-1, keepdims=True) + EPS)
            unit = raw * inverse
            weighted = total(r, slice(2 * at, 2 * at + head_dim)) * gain
            grad = inverse * (weighted - unit * jnp.mean(weighted * unit, axis=-1, keepdims=True))
            out_ref[pl.ds(start, rows), at : at + head_dim] = grad.astype(BF16)
            value = total(r, slice(2 * at + head_dim, 2 * (at + head_dim)))
            out_ref[pl.ds(start, rows), width + at : width + at + head_dim] = value.astype(BF16)


def sum_own_grads(me, gain, key_raw, arrived, samples):
    head_dim = gain.shape[0]
    all_rows, width = key_raw.shape
    whole = pl.BlockSpec(memory_space=pltpu.VMEM)
    return pl.pallas_call(
        functools.partial(own_grads_kernel, samples, head_dim),
        in_specs=[pl.BlockSpec(memory_space=pltpu.SMEM)] + [whole] * (2 + len(arrived)),
        out_specs=whole,
        out_shape=jax.ShapeDtypeStruct((all_rows, 2 * width), BF16),
        cost_estimate=pl.CostEstimate(
            flops=40 * all_rows * width * len(arrived), bytes_accessed=4 * all_rows * width * 5, transcendentals=0
        ),
        name="own_grads",
    )(me, gain.reshape(1, head_dim), key_raw, *arrived)


def pack_kernel(samples, where_ref, *refs):
    blocks, (stay_ref, go_ref) = refs[:-2], refs[-2:]
    x = lax.rem(where_ref[2], samples)
    rows, share = blocks[0].shape[0], stay_ref.shape[1]
    for z, block in enumerate(blocks):
        span = slice(z * rows, (z + 1) * rows)
        stay_ref[span, :] = block[:, pl.ds(pl.multiple_of(x * share, 128), share)]
        go_ref[span, :] = block[:, pl.ds(pl.multiple_of((samples - 1 - x) * share, 128), share)]


def pack(where, blocks, samples):
    rows, width = blocks[0].shape
    whole = pl.BlockSpec(memory_space=pltpu.VMEM)
    shape = jax.ShapeDtypeStruct((len(blocks) * rows, width // samples), BF16)
    return pl.pallas_call(
        functools.partial(pack_kernel, samples),
        in_specs=[pl.BlockSpec(memory_space=pltpu.SMEM)] + [whole] * len(blocks),
        out_specs=[whole] * 2,
        out_shape=[shape] * 2,
        cost_estimate=pl.CostEstimate(
            flops=0, bytes_accessed=4 * len(blocks) * rows * width, transcendentals=0
        ),
        name="pack",
    )(where, *blocks)


def weight_kernel(n, dps, samples, where_ref, *refs):
    vision, grads, refs = refs[:4], refs[4 : n + 4], refs[n + 4 :]
    keep_ref, sent_refs = refs[0], refs[1:dps]
    vision_all, grads_all = refs[dps:]
    mine, helped, me = where_ref[0], where_ref[1], where_ref[2]
    rows = vision[0].shape[0] * samples // n
    all_rows = rows * samples

    def place_of(i):
        return jnp.where(lax.rem(i, 2) == 0, lax.div(i, 2), n - 1 - lax.div(i, 2))

    for j in range(n):
        k = lax.rem(place_of(me) + n - place_of(lax.bitwise_xor(me, j)), n)
        span = slice(j // 2 * rows, (j // 2 + 1) * rows)
        here = pl.multiple_of(k * all_rows + helped * rows, 16)
        there = pl.multiple_of(k * all_rows + (samples - 1 - helped) * rows, 16)
        vision_all[pl.ds(here, rows), :] = vision[j % 2][span, :]
        vision_all[pl.ds(there, rows), :] = vision[2 + j % 2][span, :]
    for k in range(n):
        place = jnp.where(mine == 0, k, (n - k) % n)
        grads_all[pl.ds(pl.multiple_of(place * all_rows, 16), all_rows), :] = grads[k][...]
    piece = keep_ref.shape[0]
    for r in range(dps):
        cols = pl.ds(pl.multiple_of(lax.rem(mine + r, dps) * piece, 128), piece)
        part = lax.dot_general(
            vision_all[:, cols], grads_all[...], (((0,), (0,)), ((), ())), preferred_element_type=F32
        )
        if r == 0:
            keep_ref[...] = part
        else:
            sent_refs[r - 1][...] = part.astype(BF16)


def weight_grads(where, vision, grads, n, dps, samples):
    share = vision[0].shape[1]
    all_rows = vision[0].shape[0] * samples * samples // n
    width = grads[0].shape[1]
    piece = share // dps
    whole = pl.BlockSpec(memory_space=pltpu.VMEM)
    inputs = [*vision, *grads]
    return pl.pallas_call(
        functools.partial(weight_kernel, n, dps, samples),
        in_specs=[pl.BlockSpec(memory_space=pltpu.SMEM)] + [whole] * len(inputs),
        out_specs=[whole] * dps,
        out_shape=[jax.ShapeDtypeStruct((piece, width), F32)]
        + [jax.ShapeDtypeStruct((piece, width), BF16)] * (dps - 1),
        scratch_shapes=[pltpu.VMEM((n * all_rows, share), BF16), pltpu.VMEM((n * all_rows, width), BF16)],
        cost_estimate=pl.CostEstimate(
            flops=2 * n * all_rows * share * width,
            bytes_accessed=2 * n * all_rows * (share + width),
            transcendentals=0,
        ),
        name="weight_grads",
    )(where, *inputs)


def scatter_kernel(pieces, n, share, where_ref, *refs):
    piece_refs, refs = refs[: len(pieces)], refs[len(pieces) :]
    outs, wide, sem = refs[-4:-2], refs[-2], refs[-1]
    half = outs[0].shape[1]
    at, mine = where_ref[0], where_ref[1]
    copies = []
    top = 0
    for p, (steps, side, core, below) in enumerate(pieces):
        rows = piece_refs[p].shape[0]
        place = lax.rem(at + n + steps + side * mine, n)
        core_at = lax.rem(mine + core, 2)
        device = jnp.where(place < n // 2, 2 * place, 2 * (n - 1 - place) + 1)
        start = pl.multiple_of(device * share + core_at * (share // 2) + below, 8)
        for q, out in enumerate(outs):
            wide[q, top : top + rows, :] = piece_refs[p][:, q * half : (q + 1) * half].astype(F32)
            copy = pltpu.make_async_copy(
                wide.at[q, pl.ds(top, rows), :], out.at[pl.ds(start, rows), :], sem.at[p, q]
            )
            copy.start()
            copies.append(copy)
        top += rows
    for copy in copies:
        copy.wait()


def scatter_rows(outs, where, values, pieces, n):
    count = len(values)
    rows = sum(v.shape[0] for v in values)
    width = values[0].shape[1] // 2
    whole = pl.BlockSpec(memory_space=pltpu.VMEM)
    share = outs[0].shape[0] // n
    return pl.pallas_call(
        functools.partial(scatter_kernel, pieces, n, share),
        in_specs=[pl.BlockSpec(memory_space=pltpu.SMEM)]
        + [whole] * count
        + [pl.BlockSpec(memory_space=pl.ANY)] * 2,
        out_specs=[pl.BlockSpec(memory_space=pl.ANY)] * 2,
        scratch_shapes=[pltpu.VMEM((2, rows, width), F32), pltpu.SemaphoreType.DMA((count, 2))],
        out_shape=[jax.ShapeDtypeStruct(o.shape, F32) for o in outs],
        input_output_aliases={1 + count: 0, 2 + count: 1},
        cost_estimate=pl.CostEstimate(flops=rows * width * 2000, bytes_accessed=rows * width * 12, transcendentals=0),
        name="scatter_rows",
    )(where, *values, *outs)


def blank_kernel(*refs):
    pass


def blank(shape):
    return pl.pallas_call(
        blank_kernel,
        out_specs=[pl.BlockSpec(memory_space=pl.ANY)] * 2,
        out_shape=[jax.ShapeDtypeStruct(shape, F32)] * 2,
        name="blank",
    )()


def local(sizes, queries, vision, key_weight, value_weight, query_gain, key_gain, out_grad, tile_count):
    n, dps, mps = sizes["seq"], sizes["dp"], sizes["mp"]
    head_dim = query_gain.shape[0]
    samples, rows, model = vision.shape
    width = key_weight.shape[1]
    me, mine, mp = lax.axis_index("seq"), lax.axis_index("dp"), lax.axis_index("mp")
    x = me % samples
    me_ref = me.astype(jnp.int32).reshape(1)
    order = [i for i in range(0, n, 2)] + [i for i in range(n - 1, 0, -2)]
    helped = mp % samples

    assert n & (n - 1) == 0 and samples == 2
    far_first = sorted(range(1, n), key=lambda j: (-((j // 2).bit_length()), -(j // 2), j % 2))

    def swap(value, j):
        return lax.ppermute(value, "seq", [(i, i ^ j) for i in range(n)])

    def place_of(i):
        return jnp.where(i % 2 == 0, i // 2, n - 1 - i // 2)

    def within(value, axis, k, size):
        perm = [(i, i // samples * samples + (i % samples + k) % samples) for i in range(size)]
        return lax.ppermute(value, axis, perm)

    def pick(value, i):
        return lax.dynamic_index_in_dim(value, i % samples, 0, False)

    flat_vision = vision.reshape(samples * rows, model)
    kv_here = width // head_dim
    chunks = chunks_of()
    key_raw, kv_rel = project(me_ref, key_gain, flat_vision, key_weight, value_weight, samples, chunks)
    kv_blocks = []
    for c in range(chunks):
        pair = swap(kv_rel[1][c], 1)
        blocks = [kv_rel[0][c], pair] + [None] * (n - 2)
        for z, step in doubling(n // 2):
            blocks[2 * z] = swap(blocks[2 * (z - step)], 2 * step)
            blocks[2 * z + 1] = swap(blocks[2 * (z - step) + 1], 2 * step)
        kv_blocks.append(blocks)

    others = swap(jnp.concatenate([pick(queries, x + 1), pick(out_grad, x + 1)], axis=0), 1)

    share = model // n
    at = place_of(me)
    where = jnp.stack([mine, helped, me]).astype(jnp.int32)
    sample_vision = pick(vision, helped)

    def cut(z):
        return lax.dynamic_slice_in_dim(sample_vision, z * samples * share, samples * share, axis=1)

    lines = [cut(me // 2)] + [None] * (n // 2 - 1)
    for z in range(n // 2 - 1, 0, -1):
        lines[z] = swap(cut(me // 2 ^ z), 2 * z)

    results = []
    for c in range(chunks):
        results = attention(
            me_ref, tile_count, query_gain, queries, out_grad, others, kv_blocks[c], head_dim,
            kv_here, c * kv_here // chunks, results,
        )
    dq, dkv = results[:2], results[2:]

    arrived = [dkv[0]] + [None] * (n - 1)
    for j in far_first:
        arrived[j] = swap(dkv[j], j)
    returned = within(dq[1], "seq", 1, n)
    vision_near, going = pack(where, lines, samples)
    vision_far = swap(going, 1)
    cross_near = within(vision_near, "mp", 1, mps)
    cross_far = within(vision_far, "mp", 1, mps)
    vision_rows = [vision_near, vision_far, cross_near, cross_far]
    own_grads = sum_own_grads(me_ref, key_gain, key_raw, arrived, samples)

    def across(value):
        return lax.ppermute(value, "dp", [(i, (i + 1) % dps) for i in range(dps)])

    def split_ring(value):
        perm = []
        for d in range(dps):
            perm += [(d * n + order[i], d * n + order[(i + 1 - 2 * d) % n]) for i in range(n)]
        return lax.ppermute(value, ("dp", "seq"), perm)

    grads = [own_grads] + [None] * (n - 1)
    held = [own_grads, across(own_grads)]
    for k in range(1, n // 2):
        held = [split_ring(v) for v in held]
        grads[k], grads[n - k] = held[0], across(held[1])
    grads[n // 2] = split_ring(held[0])

    over_cols = (((1,), (1,)), ((), ()))
    full = lax.dot_general(own_grads[:, :width], key_weight, over_cols, preferred_element_type=F32)
    full = full + lax.dot_general(own_grads[:, width:], value_weight, over_cols, preferred_element_type=F32)
    cols = model // mps
    slices = [lax.dynamic_slice_in_dim(full, (mp + k) % mps * cols, cols, axis=1) for k in range(mps)]
    slices = [slices[0]] + [v.astype(BF16) for v in slices[1:]]
    vision_rows, slices = lax.optimization_barrier((vision_rows, slices))
    received = []
    for k in range(1, mps):
        received.append(lax.ppermute(slices[k], "mp", [(i, (i + k) % mps) for i in range(mps)]))
    vision_grad = slices[0]
    for got in received:
        vision_grad = vision_grad + got.astype(F32)
    vision_grad = vision_grad.astype(BF16).reshape(samples, rows, cols)

    keep, sent = weight_grads(where, vision_rows, grads, n, dps, samples)

    shard = (keep + across(sent).astype(F32)).astype(BF16)
    spot = jnp.stack([at, mine]).astype(jnp.int32)
    query_grad = lax.dynamic_update_index_in_dim(dq[0], returned, (x + 1) % samples, 0)
    values = [shard, across(shard)]
    outs = blank((model, width))
    outs = scatter_rows(outs, spot, values, ((0, 0, 0, 0), (0, 0, 1, 0)), n)
    far = n // 2
    for k in range(1, far + 1):
        for _ in range(dps if k < far else 1):
            values.append(split_ring(values[-dps]))
        new = values[-dps:] if k < far else values[-1:]
        pieces = tuple((-k, 2 * k, core, 0) for core in range(len(new)))
        pieces += tuple((k, -2 * k, 1 - core, 0) for core in range(len(new)))
        crossing = [across(v) for v in new]
        outs = scatter_rows(outs, spot, list(new) + crossing, pieces, n)
    key_weight_grad, value_weight_grad = outs

    query_grad = lax.dynamic_update_index_in_dim(dq[0], returned, (x + 1) % samples, 0)
    return (query_grad, vision_grad, key_weight_grad, value_weight_grad)


def doubling(size):
    found = [0]
    step = size // 2
    moves = []
    while step:
        moves += [(z + step, step) for z in found]
        found += [z + step for z in found]
        step //= 2
    return moves


def chunks_of():
    return 1


def solution(mesh):
    in_specs = (
        P("dp", "seq", "mp"),
        P("dp", "seq", None),
        P(None, "mp"),
        P(None, "mp"),
        P(),
        P(),
        P("dp", "seq", "mp"),
        P("dp"),
    )
    out_specs = (P("dp", "seq", "mp"), P("dp", "seq", "mp"), P(None, "mp"), P(None, "mp"))

    def body(*args):
        return local(dict(mesh.shape), *args)

    step = jax.shard_map(body, mesh=mesh, in_specs=in_specs, out_specs=out_specs, check_vma=False)
    return lambda *args: step(*args)
```

```python
import functools
import math

import jax
import jax.numpy as jnp
from jax import lax
from jax.experimental import pallas as pl
from jax.experimental.pallas import tpu as pltpu
from jax.sharding import PartitionSpec as P


MAX_TILES = 4
EPS = 1e-05
NEG = -1e30
F32 = jnp.float32
BF16 = jnp.bfloat16


def attention_kernel(blocks, parts, group, head_dim, me_ref, tiles_ref, gain_ref, *refs):
    q_refs, refs = refs[:parts], refs[parts:]
    g_refs, refs = refs[:parts], refs[parts:]
    kv_refs, refs = refs[:blocks], refs[-(parts + blocks + 4) :]
    dq_refs, refs = refs[:parts], refs[parts:]
    dkv_refs, refs = refs[:blocks], refs[blocks:]
    keys, values, dkeys, dvalues = refs
    dq_refs = [dq_refs[0].at[0]] + list(dq_refs[1:])
    rows = kv_refs[0].shape[0]
    total = rows * blocks
    scale = head_dim ** (-0.5)
    token = lax.broadcasted_iota(jnp.int32, (total, 1), 0)
    live = token < 0
    me = me_ref[0]
    live_end = tiles_ref[lax.rem(me, parts)] * (total // MAX_TILES)
    for k in range(blocks):
        keys[k * rows : (k + 1) * rows, :] = kv_refs[k][:, :head_dim]
        values[k * rows : (k + 1) * rows, :] = kv_refs[k][:, head_dim:]
        start = k * rows
        left = live_end - lax.bitwise_xor(me, k) * rows
        live = live | ((token >= start) & (token < start + jnp.minimum(left, rows)))
    bias = jnp.where(live, 0.0, NEG)
    gain = gain_ref[...]
    keys_all = keys[...]
    values_all = values[...]
    keys_turned = keys_all.T
    values_turned = values_all.T
    over_dims = (((1,), (1,)), ((), ()))

    def front(h):
        cols = slice(h * head_dim, (h + 1) * head_dim)
        raw_b = jnp.concatenate([ref[..., cols].reshape(-1, head_dim) for ref in q_refs], axis=0)
        out_b = jnp.concatenate([ref[..., cols].reshape(-1, head_dim) for ref in g_refs], axis=0)
        raw = raw_b.astype(F32)
        inverse = lax.rsqrt(jnp.mean(raw * raw, axis=-1, keepdims=True) + EPS)
        unit = raw * inverse
        normed = (unit * gain).astype(BF16)
        scores = lax.dot_general(keys_all, normed, over_dims, preferred_element_type=F32)
        dprobs = lax.dot_general(values_all, out_b, over_dims, preferred_element_type=F32)
        return cols, out_b, inverse, unit, normed, scores, dprobs

    def middle(cols, out_b, inverse, unit, normed, scores, dprobs):
        scores = scores * (scale * math.log2(math.e)) + bias
        expo = jnp.exp2(scores - jnp.max(scores, axis=0, keepdims=True))
        probs = expo * (1.0 / jnp.sum(expo, axis=0, keepdims=True))
        probs_b = probs.astype(BF16)
        attn = jnp.dot(values_turned, probs_b, preferred_element_type=F32).astype(BF16)
        delta = jnp.sum(out_b.T.astype(F32) * attn.astype(F32), axis=0, keepdims=True)
        dscores = (probs * (dprobs - delta)).astype(BF16)
        return cols, out_b, inverse, unit, normed, probs_b, dscores

    def back(h, cols, out_b, inverse, unit, normed, probs_b, dscores):
        dnormed = jnp.dot(keys_turned, dscores, preferred_element_type=F32).T * scale
        weighted = dnormed * gain
        grad = inverse * (weighted - unit * jnp.mean(weighted * unit, axis=-1, keepdims=True))
        grad = grad.astype(BF16)
        part_rows = grad.shape[0] // parts
        for p in range(parts):
            dq_refs[p][:, cols] = grad[p * part_rows : (p + 1) * part_rows]
        dk = jnp.dot(dscores, normed, preferred_element_type=F32)
        dv = jnp.dot(probs_b, out_b, preferred_element_type=F32)
        if h == 0:
            dkeys[...] = dk
            dvalues[...] = dv
        else:
            dkeys[...] += dk
            dvalues[...] += dv

    ahead = front(0)
    behind = None
    for h in range(group):
        now = ahead
        if h + 1 < group:
            ahead = front(h + 1)
        mid = middle(*now)
        if behind is not None:
            back(h - 1, *behind)
        behind = mid
    back(group - 1, *behind)
    for k in range(blocks):
        span = slice(k * rows, (k + 1) * rows)
        dkv_refs[k][:, :head_dim] = (dkeys[span, :] * scale).astype(BF16)
        dkv_refs[k][:, head_dim:] = dvalues[span, :].astype(BF16)


def attention(me, tiles, gain, queries, out_grad, others, kv_blocks, head_dim, kv_here, first, before):
    blocks = len(kv_blocks)
    parts = 2
    text_rows, width = queries.shape[1:]
    rows, kv_width = kv_blocks[0].shape
    heads = kv_width // (2 * head_dim)
    group = width // head_dim // kv_here
    group_width = group * head_dim
    total = rows * blocks
    own = pl.BlockSpec((1, text_rows, group_width), lambda g, m, t: (lax.rem(m[0], parts), 0, g + first))
    other = pl.BlockSpec((text_rows, group_width), lambda g, m, t: (0, g + first))
    below = pl.BlockSpec((text_rows, group_width), lambda g, m, t: (1, g + first))
    kv = pl.BlockSpec((rows, 2 * head_dim), lambda g, m, t: (0, g))
    dkv = pl.BlockSpec((rows, 2 * head_dim), lambda g, m, t: (0, g + first))
    gain_spec = pl.BlockSpec((1, head_dim), lambda g, m, t: (0, 0))
    work = text_rows * parts * group * heads * total
    results = pl.pallas_call(
        functools.partial(attention_kernel, blocks, parts, group, head_dim),
        grid_spec=pltpu.PrefetchScalarGridSpec(
            num_scalar_prefetch=2,
            grid=(heads,),
            in_specs=[gain_spec, own, other, own, below]
            + [kv] * blocks
            + [pl.BlockSpec(memory_space=pl.ANY)] * len(before),
            out_specs=[own, other] + [dkv] * blocks,
            scratch_shapes=[pltpu.VMEM((total, head_dim), BF16)] * 2
            + [pltpu.VMEM((total, head_dim), F32)] * 2,
        ),
        out_shape=[jax.ShapeDtypeStruct(queries.shape, BF16), jax.ShapeDtypeStruct((text_rows, width), BF16)]
        + [jax.ShapeDtypeStruct((rows, 2 * head_dim * kv_here), BF16)] * blocks,
        input_output_aliases={7 + blocks + i: i for i in range(len(before))},
        cost_estimate=pl.CostEstimate(
            flops=12 * work * head_dim,
            bytes_accessed=6 * text_rows * parts * group_width * heads,
            transcendentals=work,
        ),
        name="attention",
    )(me, tiles, gain.reshape(1, head_dim), queries, others, out_grad, others, *kv_blocks, *before)
    return results


def project_kernel(samples, chunks, head_dim, me_ref, gain_ref, vision_ref, key_ref, value_ref, *refs):
    raw_ref, kv_refs, (keys, values) = refs[0], refs[1:-2], refs[-2:]
    step = pl.program_id(0)
    vision = vision_ref[...]
    key_part = jnp.dot(vision, key_ref[...], preferred_element_type=F32)
    value_part = jnp.dot(vision, value_ref[...], preferred_element_type=F32)

    @pl.when(step == 0)
    def _():
        keys[...] = key_part
        values[...] = value_part

    @pl.when(step > 0)
    def _():
        keys[...] += key_part
        values[...] += value_part

    @pl.when(step == pl.num_programs(0) - 1)
    def _():
        raw_ref[...] = keys[...]
        gain = gain_ref[...]
        rows = kv_refs[0].shape[0]
        x = lax.rem(me_ref[0], samples)
        for r in range(samples):
            start = pl.multiple_of(lax.rem(x + r, samples) * rows, 8)
            heads = keys.shape[1] // head_dim
            for h in range(heads):
                cols = slice(h * head_dim, (h + 1) * head_dim)
                raw = keys[pl.ds(start, rows), cols]
                inverse = lax.rsqrt(jnp.mean(raw * raw, axis=-1, keepdims=True) + EPS)
                kv_ref = kv_refs[r * chunks + h * chunks // heads]
                at = 2 * (h % (heads // chunks)) * head_dim
                kv_ref[:, at : at + head_dim] = (raw * inverse * gain).astype(BF16)
                kv_ref[:, at + head_dim : at + 2 * head_dim] = values[pl.ds(start, rows), cols].astype(BF16)


def project(me, gain, vision, key_weight, value_weight, samples, chunks):
    all_rows, model = vision.shape
    width = key_weight.shape[1]
    head_dim = gain.shape[0]
    rows = all_rows // samples
    step = math.gcd(model, 2048)
    weight = pl.BlockSpec((step, width), lambda i, m: (i, 0))
    results = pl.pallas_call(
        functools.partial(project_kernel, samples, chunks, head_dim),
        grid_spec=pltpu.PrefetchScalarGridSpec(
            num_scalar_prefetch=1,
            grid=(model // step,),
            in_specs=[
                pl.BlockSpec((1, head_dim), lambda i, m: (0, 0)),
                pl.BlockSpec((all_rows, step), lambda i, m: (0, i)),
                weight,
                weight,
            ],
            out_specs=[pl.BlockSpec((all_rows, width), lambda i, m: (0, 0))]
            + [pl.BlockSpec((rows, 2 * width // chunks), lambda i, m: (0, 0))] * (samples * chunks),
            scratch_shapes=[pltpu.VMEM((all_rows, width), F32)] * 2,
        ),
        out_shape=[jax.ShapeDtypeStruct((all_rows, width), F32)]
        + [jax.ShapeDtypeStruct((rows, 2 * width // chunks), BF16)] * (samples * chunks),
        cost_estimate=pl.CostEstimate(
            flops=4 * all_rows * model * width,
            bytes_accessed=2 * model * (all_rows + 2 * width),
            transcendentals=0,
        ),
        name="project",
    )(me, gain.reshape(1, head_dim), vision, key_weight, value_weight)
    return results[0], [results[1 + r * chunks : 1 + (r + 1) * chunks] for r in range(samples)]


def own_grads_kernel(samples, head_dim, me_ref, gain_ref, raw_ref, *refs):
    arrived, out_ref = refs[:-1], refs[-1]
    rows = arrived[0].shape[0]
    width = raw_ref.shape[1]
    gain = gain_ref[...]
    x = lax.rem(me_ref[0], samples)

    def total(r, cols):
        value = arrived[r][:, cols].astype(F32)
        for k in range(r + samples, len(arrived), samples):
            value = value + arrived[k][:, cols].astype(F32)
        return value

    for r in range(samples):
        start = pl.multiple_of(lax.rem(x + r, samples) * rows, 16)
        for h in range(width // head_dim):
            at = h * head_dim
            raw = raw_ref[pl.ds(start, rows), at : at + head_dim]
            inverse = lax.rsqrt(jnp.mean(raw * raw, axis=-1, keepdims=True) + EPS)
            unit = raw * inverse
            weighted = total(r, slice(2 * at, 2 * at + head_dim)) * gain
            grad = inverse * (weighted - unit * jnp.mean(weighted * unit, axis=-1, keepdims=True))
            out_ref[pl.ds(start, rows), at : at + head_dim] = grad.astype(BF16)
            value = total(r, slice(2 * at + head_dim, 2 * (at + head_dim)))
            out_ref[pl.ds(start, rows), width + at : width + at + head_dim] = value.astype(BF16)


def sum_own_grads(me, gain, key_raw, arrived, samples):
    head_dim = gain.shape[0]
    all_rows, width = key_raw.shape
    whole = pl.BlockSpec(memory_space=pltpu.VMEM)
    return pl.pallas_call(
        functools.partial(own_grads_kernel, samples, head_dim),
        in_specs=[pl.BlockSpec(memory_space=pltpu.SMEM)] + [whole] * (2 + len(arrived)),
        out_specs=whole,
        out_shape=jax.ShapeDtypeStruct((all_rows, 2 * width), BF16),
        cost_estimate=pl.CostEstimate(
            flops=40 * all_rows * width * len(arrived), bytes_accessed=4 * all_rows * width * 5, transcendentals=0
        ),
        name="own_grads",
    )(me, gain.reshape(1, head_dim), key_raw, *arrived)


def pack_kernel(samples, where_ref, *refs):
    blocks, (stay_ref, go_ref) = refs[:-2], refs[-2:]
    x = lax.rem(where_ref[2], samples)
    rows, share = blocks[0].shape[0], stay_ref.shape[1]
    for z, block in enumerate(blocks):
        span = slice(z * rows, (z + 1) * rows)
        stay_ref[span, :] = block[:, pl.ds(pl.multiple_of(x * share, 128), share)]
        go_ref[span, :] = block[:, pl.ds(pl.multiple_of((samples - 1 - x) * share, 128), share)]


def pack(where, blocks, samples):
    rows, width = blocks[0].shape
    whole = pl.BlockSpec(memory_space=pltpu.VMEM)
    shape = jax.ShapeDtypeStruct((len(blocks) * rows, width // samples), BF16)
    return pl.pallas_call(
        functools.partial(pack_kernel, samples),
        in_specs=[pl.BlockSpec(memory_space=pltpu.SMEM)] + [whole] * len(blocks),
        out_specs=[whole] * 2,
        out_shape=[shape] * 2,
        cost_estimate=pl.CostEstimate(
            flops=0, bytes_accessed=4 * len(blocks) * rows * width, transcendentals=0
        ),
        name="pack",
    )(where, *blocks)


def weight_kernel(n, dps, samples, where_ref, *refs):
    vision, grads, refs = refs[:4], refs[4 : n + 4], refs[n + 4 :]
    keep_ref, sent_refs = refs[0], refs[1:dps]
    vision_all, grads_all = refs[dps:]
    mine, helped, me = where_ref[0], where_ref[1], where_ref[2]
    rows = vision[0].shape[0] * samples // n
    all_rows = rows * samples

    def place_of(i):
        return jnp.where(lax.rem(i, 2) == 0, lax.div(i, 2), n - 1 - lax.div(i, 2))

    for j in range(n):
        k = lax.rem(place_of(me) + n - place_of(lax.bitwise_xor(me, j)), n)
        span = slice(j // 2 * rows, (j // 2 + 1) * rows)
        here = pl.multiple_of(k * all_rows + helped * rows, 16)
        there = pl.multiple_of(k * all_rows + (samples - 1 - helped) * rows, 16)
        vision_all[pl.ds(here, rows), :] = vision[j % 2][span, :]
        vision_all[pl.ds(there, rows), :] = vision[2 + j % 2][span, :]
    for k in range(n):
        place = jnp.where(mine == 0, k, (n - k) % n)
        grads_all[pl.ds(pl.multiple_of(place * all_rows, 16), all_rows), :] = grads[k][...]
    piece = keep_ref.shape[0]
    for r in range(dps):
        cols = pl.ds(pl.multiple_of(lax.rem(mine + r, dps) * piece, 128), piece)
        part = lax.dot_general(
            vision_all[:, cols], grads_all[...], (((0,), (0,)), ((), ())), preferred_element_type=F32
        )
        if r == 0:
            keep_ref[...] = part
        else:
            sent_refs[r - 1][...] = part.astype(BF16)


def weight_grads(where, vision, grads, n, dps, samples):
    share = vision[0].shape[1]
    all_rows = vision[0].shape[0] * samples * samples // n
    width = grads[0].shape[1]
    piece = share // dps
    whole = pl.BlockSpec(memory_space=pltpu.VMEM)
    inputs = [*vision, *grads]
    return pl.pallas_call(
        functools.partial(weight_kernel, n, dps, samples),
        in_specs=[pl.BlockSpec(memory_space=pltpu.SMEM)] + [whole] * len(inputs),
        out_specs=[whole] * dps,
        out_shape=[jax.ShapeDtypeStruct((piece, width), F32)]
        + [jax.ShapeDtypeStruct((piece, width), BF16)] * (dps - 1),
        scratch_shapes=[pltpu.VMEM((n * all_rows, share), BF16), pltpu.VMEM((n * all_rows, width), BF16)],
        cost_estimate=pl.CostEstimate(
            flops=2 * n * all_rows * share * width,
            bytes_accessed=2 * n * all_rows * (share + width),
            transcendentals=0,
        ),
        name="weight_grads",
    )(where, *inputs)


def scatter_kernel(pieces, n, share, where_ref, *refs):
    piece_refs, refs = refs[: len(pieces)], refs[len(pieces) :]
    outs, wide, sem = refs[-4:-2], refs[-2], refs[-1]
    half = outs[0].shape[1]
    at, mine = where_ref[0], where_ref[1]
    copies = []
    top = 0
    for p, (steps, side, core, below) in enumerate(pieces):
        rows = piece_refs[p].shape[0]
        place = lax.rem(at + n + steps + side * mine, n)
        core_at = lax.rem(mine + core, 2)
        device = jnp.where(place < n // 2, 2 * place, 2 * (n - 1 - place) + 1)
        start = pl.multiple_of(device * share + core_at * (share // 2) + below, 8)
        for q, out in enumerate(outs):
            wide[q, top : top + rows, :] = piece_refs[p][:, q * half : (q + 1) * half].astype(F32)
            copy = pltpu.make_async_copy(
                wide.at[q, pl.ds(top, rows), :], out.at[pl.ds(start, rows), :], sem.at[p, q]
            )
            copy.start()
            copies.append(copy)
        top += rows
    for copy in copies:
        copy.wait()


def scatter_rows(outs, where, values, pieces, n):
    count = len(values)
    rows = sum(v.shape[0] for v in values)
    width = values[0].shape[1] // 2
    whole = pl.BlockSpec(memory_space=pltpu.VMEM)
    share = outs[0].shape[0] // n
    return pl.pallas_call(
        functools.partial(scatter_kernel, pieces, n, share),
        in_specs=[pl.BlockSpec(memory_space=pltpu.SMEM)]
        + [whole] * count
        + [pl.BlockSpec(memory_space=pl.ANY)] * 2,
        out_specs=[pl.BlockSpec(memory_space=pl.ANY)] * 2,
        scratch_shapes=[pltpu.VMEM((2, rows, width), F32), pltpu.SemaphoreType.DMA((count, 2))],
        out_shape=[jax.ShapeDtypeStruct(o.shape, F32) for o in outs],
        input_output_aliases={1 + count: 0, 2 + count: 1},
        cost_estimate=pl.CostEstimate(flops=rows * width * 2000, bytes_accessed=rows * width * 12, transcendentals=0),
        name="scatter_rows",
    )(where, *values, *outs)


def blank_kernel(*refs):
    pass


def blank(shape):
    return pl.pallas_call(
        blank_kernel,
        out_specs=[pl.BlockSpec(memory_space=pl.ANY)] * 2,
        out_shape=[jax.ShapeDtypeStruct(shape, F32)] * 2,
        name="blank",
    )()


def local(sizes, queries, vision, key_weight, value_weight, query_gain, key_gain, out_grad, tile_count):
    n, dps, mps = sizes["seq"], sizes["dp"], sizes["mp"]
    head_dim = query_gain.shape[0]
    samples, rows, model = vision.shape
    width = key_weight.shape[1]
    me, mine, mp = lax.axis_index("seq"), lax.axis_index("dp"), lax.axis_index("mp")
    x = me % samples
    me_ref = me.astype(jnp.int32).reshape(1)
    order = [i for i in range(0, n, 2)] + [i for i in range(n - 1, 0, -2)]
    helped = mp % samples

    assert n & (n - 1) == 0 and samples == 2
    far_first = sorted(range(1, n), key=lambda j: (-((j // 2).bit_length()), -(j // 2), j % 2))

    def swap(value, j):
        return lax.ppermute(value, "seq", [(i, i ^ j) for i in range(n)])

    def place_of(i):
        return jnp.where(i % 2 == 0, i // 2, n - 1 - i // 2)

    def within(value, axis, k, size):
        perm = [(i, i // samples * samples + (i % samples + k) % samples) for i in range(size)]
        return lax.ppermute(value, axis, perm)

    def pick(value, i):
        return lax.dynamic_index_in_dim(value, i % samples, 0, False)

    flat_vision = vision.reshape(samples * rows, model)
    kv_here = width // head_dim
    chunks = chunks_of()
    key_raw, kv_rel = project(me_ref, key_gain, flat_vision, key_weight, value_weight, samples, chunks)
    kv_blocks = []
    for c in range(chunks):
        pair = swap(kv_rel[1][c], 1)
        blocks = [kv_rel[0][c], pair] + [None] * (n - 2)
        for z, step in doubling(n // 2):
            blocks[2 * z] = swap(blocks[2 * (z - step)], 2 * step)
            blocks[2 * z + 1] = swap(blocks[2 * (z - step) + 1], 2 * step)
        kv_blocks.append(blocks)

    others = swap(jnp.concatenate([pick(queries, x + 1), pick(out_grad, x + 1)], axis=0), 1)

    share = model // n
    at = place_of(me)
    where = jnp.stack([mine, helped, me]).astype(jnp.int32)
    sample_vision = pick(vision, helped)

    def cut(z):
        return lax.dynamic_slice_in_dim(sample_vision, z * samples * share, samples * share, axis=1)

    lines = [cut(me // 2)] + [None] * (n // 2 - 1)
    for z in range(n // 2 - 1, 0, -1):
        lines[z] = swap(cut(me // 2 ^ z), 2 * z)

    results = []
    for c in range(chunks):
        results = attention(
            me_ref, tile_count, query_gain, queries, out_grad, others, kv_blocks[c], head_dim,
            kv_here, c * kv_here // chunks, results,
        )
    dq, dkv = results[:2], results[2:]

    arrived = [dkv[0]] + [None] * (n - 1)
    for j in far_first:
        arrived[j] = swap(dkv[j], j)
    returned = within(dq[1], "seq", 1, n)
    vision_near, going = pack(where, lines, samples)
    vision_far = swap(going, 1)
    cross_near = within(vision_near, "mp", 1, mps)
    cross_far = within(vision_far, "mp", 1, mps)
    vision_rows = [vision_near, vision_far, cross_near, cross_far]
    own_grads = sum_own_grads(me_ref, key_gain, key_raw, arrived, samples)

    def across(value):
        return lax.ppermute(value, "dp", [(i, (i + 1) % dps) for i in range(dps)])

    def split_ring(value):
        perm = []
        for d in range(dps):
            perm += [(d * n + order[i], d * n + order[(i + 1 - 2 * d) % n]) for i in range(n)]
        return lax.ppermute(value, ("dp", "seq"), perm)

    grads = [own_grads] + [None] * (n - 1)
    held = [own_grads, across(own_grads)]
    for k in range(1, n // 2):
        for core in range(dps):
            held[core] = split_ring(held[core])
        grads[k], grads[n - k] = held[0], across(held[1])
    grads[n // 2] = split_ring(held[0])

    over_cols = (((1,), (1,)), ((), ()))
    full = lax.dot_general(own_grads[:, :width], key_weight, over_cols, preferred_element_type=F32)
    full = full + lax.dot_general(own_grads[:, width:], value_weight, over_cols, preferred_element_type=F32)
    cols = model // mps
    slices = [lax.dynamic_slice_in_dim(full, (mp + k) % mps * cols, cols, axis=1) for k in range(mps)]
    slices = [slices[0]] + [v.astype(BF16) for v in slices[1:]]
    received = []
    for k in range(1, mps):
        received.append(lax.ppermute(slices[k], "mp", [(i, (i + k) % mps) for i in range(mps)]))
    vision_grad = slices[0]
    for got in received:
        vision_grad = vision_grad + got.astype(F32)
    vision_grad = vision_grad.astype(BF16).reshape(samples, rows, cols)

    keep, sent = weight_grads(where, vision_rows, grads, n, dps, samples)

    shard = (keep + across(sent).astype(F32)).astype(BF16)
    spot = jnp.stack([at, mine]).astype(jnp.int32)
    query_grad = lax.dynamic_update_index_in_dim(dq[0], returned, (x + 1) % samples, 0)
    values = [shard, across(shard)]
    outs = blank((model, width))
    outs = scatter_rows(outs, spot, values, ((0, 0, 0, 0), (0, 0, 1, 0)), n)
    far = n // 2
    for k in range(1, far + 1):
        for _ in range(dps if k < far else 1):
            values.append(split_ring(values[-dps]))
        new = values[-dps:] if k < far else values[-1:]
        pieces = tuple((-k, 2 * k, core, 0) for core in range(len(new)))
        pieces += tuple((k, -2 * k, 1 - core, 0) for core in range(len(new)))
        crossing = [across(v) for v in new]
        outs = scatter_rows(outs, spot, list(new) + crossing, pieces, n)
    key_weight_grad, value_weight_grad = outs

    query_grad = lax.dynamic_update_index_in_dim(dq[0], returned, (x + 1) % samples, 0)
    return (query_grad, vision_grad, key_weight_grad, value_weight_grad)


def doubling(size):
    found = [0]
    step = size // 2
    moves = []
    while step:
        moves += [(z + step, step) for z in found]
        found += [z + step for z in found]
        step //= 2
    return moves


def chunks_of():
    return 1


def solution(mesh):
    in_specs = (
        P("dp", "seq", "mp"),
        P("dp", "seq", None),
        P(None, "mp"),
        P(None, "mp"),
        P(),
        P(),
        P("dp", "seq", "mp"),
        P("dp"),
    )
    out_specs = (P("dp", "seq", "mp"), P("dp", "seq", "mp"), P(None, "mp"), P(None, "mp"))

    def body(*args):
        return local(dict(mesh.shape), *args)

    step = jax.shard_map(body, mesh=mesh, in_specs=in_specs, out_specs=out_specs, check_vma=False)
    return lambda *args: step(*args)
```
